128 devices in a mesh: dp: 2 (over core), fsdp: 64 (over z, y, x).
Axes of the slice: x: 4, y: 4, z: 4, core: 2. Of those that a mesh axis runs over, the one named last changes fastest.
Arguments:
- master: float32 [1, 13075328], P(None, ('dp', 'fsdp'))
- adam_m: float32 [1, 13075328], P(None, ('dp', 'fsdp'))
- adam_v: float32 [1, 13075328], P(None, ('dp', 'fsdp'))
- inputs: bfloat16 [1, 512, 256, 896], P(None, ('dp', 'fsdp'))
- targets: bfloat16 [1, 512, 256, 896], P(None, ('dp', 'fsdp'))
Outputs:
- output 1: float32 [1, 13075328], P(None, ('dp', 'fsdp'))
- output 2: float32 [1, 13075328], P(None, ('dp', 'fsdp'))
- output 3: float32 [1, 13075328], P(None, ('dp', 'fsdp'))
- output 4: float32 [], replicated
All inputs are finite; a program needn't handle non-finite values.
Results may differ from the reference program's by a relative error of at most 0.001.
Values are sent between devices in bfloat16 or wider.
A program may use at most 1 GiB of HBM per device.

```python
import jax
import jax.numpy as jnp
from jax import lax

D = 896
FF = 4864
LAYERS = 1
MICRO = 1
SEQ = 256
BATCH = 512
ADAM_STEP = 3
FLAT_LEN = D * (3 * FF + 1)
TOKEN_TOTAL = MICRO * BATCH * SEQ
ROW_BLOCK = min(SEQ, 256)
LEARN_RATE = 2e-3
BETA_ONE = 0.9
BETA_TWO = 0.999
ADAM_EPS = 1e-8
DECAY_RATE = 0.1
RMS_EPS = 1e-5


def setup_inputs(seed: int = 0) -> dict:
    rng_keys = jax.random.split(jax.random.key(seed), 8)
    gain_rows = 1.0 + 0.2 * jax.random.normal(rng_keys[0], (LAYERS, D), jnp.float32)
    w_one = jax.random.normal(rng_keys[1], (LAYERS, D * FF), jnp.float32) * D ** -0.5
    w_three = jax.random.normal(rng_keys[2], (LAYERS, D * FF), jnp.float32) * D ** -0.5
    w_two = 0.5 * jax.random.normal(rng_keys[3], (LAYERS, FF * D), jnp.float32) * FF ** -0.5
    master = jnp.concatenate([gain_rows, w_one, w_three, w_two], axis=1)
    grad_scale = 0.5 * TOKEN_TOTAL ** -0.5 + 0.3 * FF ** -0.5
    past_one = grad_scale * jax.random.normal(rng_keys[4], (LAYERS, FLAT_LEN), jnp.float32)
    past_two = grad_scale * jax.random.normal(rng_keys[5], (LAYERS, FLAT_LEN), jnp.float32)
    adam_m = (1.0 - BETA_ONE) * (BETA_ONE * past_one + past_two)
    adam_v = (1.0 - BETA_TWO) * (BETA_TWO * past_one * past_one + past_two * past_two)
    act_shape = (MICRO, BATCH, SEQ, D)
    inputs = jax.random.normal(rng_keys[6], act_shape, jnp.float32).astype(jnp.bfloat16)
    targets = jax.random.normal(rng_keys[7], act_shape, jnp.float32).astype(jnp.bfloat16)
    return dict(master=master, adam_m=adam_m, adam_v=adam_v, inputs=inputs, targets=targets)


def layer_forward(hidden, layer_w):
    gain_vec, w_one, w_three, w_two = layer_w
    inv_rms = lax.rsqrt(jnp.mean(hidden * hidden, axis=-1, keepdims=True) + RMS_EPS)
    normed = (hidden * inv_rms * gain_vec.astype(jnp.float32)).astype(jnp.bfloat16)
    gate_pre = jnp.dot(normed, w_one, preferred_element_type=jnp.float32)
    up_pre = jnp.dot(normed, w_three, preferred_element_type=jnp.float32)
    inner = (jax.nn.silu(gate_pre) * up_pre).astype(jnp.bfloat16)
    new_hidden = hidden + jnp.dot(inner, w_two, preferred_element_type=jnp.float32)
    return new_hidden, (hidden, gate_pre, up_pre)


def layer_backward(grad_h, layer_saved, layer_w):
    hidden, gate_pre, up_pre = layer_saved
    gain_vec, w_one, w_three, w_two = layer_w
    inv_rms = lax.rsqrt(jnp.mean(hidden * hidden, axis=-1, keepdims=True) + RMS_EPS)
    normed_f = hidden * inv_rms
    gain_f = gain_vec.astype(jnp.float32)
    normed = (normed_f * gain_f).astype(jnp.bfloat16)
    sigmoid_g = jax.nn.sigmoid(gate_pre)
    silu_g = gate_pre * sigmoid_g
    inner = (silu_g * up_pre).astype(jnp.bfloat16)
    grad_hb = grad_h.astype(jnp.bfloat16)
    d_two = jnp.dot(inner.T, grad_hb, preferred_element_type=jnp.float32)
    d_inner = jnp.dot(grad_hb, w_two.T, preferred_element_type=jnp.float32)
    d_gate = (d_inner * up_pre * sigmoid_g * (1.0 + gate_pre * (1.0 - sigmoid_g))).astype(jnp.bfloat16)
    d_up = (d_inner * silu_g).astype(jnp.bfloat16)
    d_one = jnp.dot(normed.T, d_gate, preferred_element_type=jnp.float32)
    d_three = jnp.dot(normed.T, d_up, preferred_element_type=jnp.float32)
    d_normed = jnp.dot(d_gate, w_one.T, preferred_element_type=jnp.float32) + jnp.dot(d_up, w_three.T, preferred_element_type=jnp.float32)
    d_gain = jnp.sum(d_normed * normed_f, axis=0)
    d_hn = d_normed * gain_f
    grad_prev = grad_h + inv_rms * (d_hn - normed_f * jnp.mean(d_hn * normed_f, axis=-1, keepdims=True))
    flat_grad = jnp.concatenate([d_gain, d_one.reshape(-1), d_three.reshape(-1), d_two.reshape(-1)])
    return grad_prev, flat_grad


def reference(master, adam_m, adam_v, inputs, targets):
    work = master.astype(jnp.bfloat16)
    tail_at = D + 2 * D * FF
    weights = (work[:, :D], work[:, D:D + D * FF].reshape(LAYERS, D, FF), work[:, D + D * FF:tail_at].reshape(LAYERS, D, FF), work[:, tail_at:].reshape(LAYERS, FF, D))

    def block_step(carry, block_pair):
        grad_acc, loss_acc = carry
        block_in, block_target = block_pair
        hidden_out, saved_acts = lax.scan(layer_forward, block_in.astype(jnp.float32), weights)
        residual_err = hidden_out - block_target.astype(jnp.float32)

        def back_body(grad_h, layer_pack):
            return layer_backward(grad_h, layer_pack[0], layer_pack[1])

        grad_input, flat_grads = lax.scan(back_body, residual_err, (saved_acts, weights), reverse=True)
        return (grad_acc + flat_grads, loss_acc + 0.5 * jnp.sum(residual_err * residual_err)), None

    blocks_in = inputs.reshape(TOKEN_TOTAL // ROW_BLOCK, ROW_BLOCK, D)
    blocks_target = targets.reshape(TOKEN_TOTAL // ROW_BLOCK, ROW_BLOCK, D)
    carry_init = (jnp.zeros((LAYERS, FLAT_LEN), jnp.float32), jnp.zeros((), jnp.float32))
    (grad_sum, loss_sum), block_ys = lax.scan(block_step, carry_init, (blocks_in, blocks_target))
    grad_mean = grad_sum / TOKEN_TOTAL
    m_new = BETA_ONE * adam_m + (1.0 - BETA_ONE) * grad_mean
    v_new = BETA_TWO * adam_v + (1.0 - BETA_TWO) * grad_mean * grad_mean
    m_hat = m_new / (1.0 - BETA_ONE ** ADAM_STEP)
    v_hat = v_new / (1.0 - BETA_TWO ** ADAM_STEP)
    master_new = master - LEARN_RATE * (m_hat / (jnp.sqrt(v_hat) + ADAM_EPS) + DECAY_RATE * master)
    return master_new, m_new, v_new, loss_sum / TOKEN_TOTAL
```

```python
import functools

import jax
import jax.numpy as jnp
from jax import lax
from jax.experimental import pallas as pl
from jax.experimental.pallas import tpu as pltpu
from jax.sharding import PartitionSpec as P

ADAM_STEP = 3
LEARN_RATE = 2e-3
BETA_ONE = 0.9
BETA_TWO = 0.999
ADAM_EPS = 1e-8
DECAY_RATE = 0.1
RMS_EPS = 1e-5

D = 896
FF = 4864
FLAT = D * (3 * FF + 1)
NDEV = 128
GRP = 64
SHARD = FLAT // NDEV
NB = FF // 128
ND = D // 128
HB = NB // 2
W2_START = D + 2 * D * FF
FIRST_W2 = 85
SPILL = 35840
ROWS13, ROWS2 = 24, 120
AL_LEN = ROWS13 * FF

CHUNKS = (3, 8, 8)
OFFS = (0, 3, 11)
TPD = (16, 42, 42)
SLOT0 = (0, 16, 58)
SLOTS = 100
GAIN_F = GRP - 1

MESH = pl.DeviceIdType.MESH


def row_start(dev):
    return (21 * dev + 7) // 8


def w2_row_start(dev):
    return jnp.maximum((114 * dev - 9728 + 7) // 8, 0)


def tile_of(k, c, p):
    n = CHUNKS[k]
    row13 = p // n
    col13 = HB * c + OFFS[k] + p % n
    p2 = p - 2 * (D // 8) * n
    row2 = (FF // 16) * c + 16 * OFFS[k] + p2 // ND
    col2 = p2 % ND
    return row13, col13, row2, col2


def my_index():
    return lax.axis_index('dp') * GRP + lax.axis_index('fsdp')


def move(src, dst, send_sem, recv_sem, c, f, waiting):
    stays = (c == lax.axis_index('dp')) & (f == lax.axis_index('fsdp'))

    def remote():
        return pltpu.make_async_remote_copy(
            src_ref=src, dst_ref=dst, send_sem=send_sem, recv_sem=recv_sem, device_id=(c, f), device_id_type=MESH)

    if waiting:
        @pl.when(jnp.logical_not(stays))
        def _():
            remote().wait_send()
    else:
        @pl.when(jnp.logical_not(stays))
        def _():
            remote().start()

        @pl.when(stays)
        def _():
            pltpu.make_async_copy(src, dst, recv_sem).start()


def spread_kernel(src13, src2, gain_src, out, send13, send2, send_gain, recv):
    dev = my_index()
    me_f = lax.axis_index('fsdp')

    def all_sends(waiting):
        def send(src, k, c, p, sem):
            move(src, out.at[SLOT0[k] + p % TPD[k]], sem, recv.at[k], c, p // TPD[k], waiting)

        @pl.when(dev < FIRST_W2)
        def _():
            first = row_start(dev)

            def per_row(t, carry):
                for k in range(len(CHUNKS)):
                    n = CHUNKS[k]

                    def per_col(j, carry2):
                        for c in range(2):
                            col = HB * c + OFFS[k] + j
                            send(src13.at[pl.ds(t * 8, 8), col], k, c, (first + t) * n + j, send13.at[t])
                        return carry2

                    lax.fori_loop(0, n, per_col, 0)
                return carry

            lax.fori_loop(0, row_start(dev + 1) - first, per_row, 0)

        @pl.when(dev >= FIRST_W2)
        def _():
            first = w2_row_start(dev)

            def per_row(t, carry):
                row = first + t
                c = row // (FF // 16)
                kk = row % (FF // 16)
                for k in range(len(CHUNKS)):
                    n = CHUNKS[k]

                    @pl.when((kk >= 16 * OFFS[k]) & (kk < 16 * (OFFS[k] + n)))
                    def _():
                        base = 2 * (D // 8) * n + (kk - 16 * OFFS[k]) * ND

                        def per_col(j, carry2):
                            send(src2.at[pl.ds(t * 8, 8), j], k, c, base + j, send2.at[t])
                            return carry2

                        lax.fori_loop(0, ND, per_col, 0)
                return carry

            lax.fori_loop(0, w2_row_start(dev + 1) - first, per_row, 0)

        @pl.when(dev == 0)
        def _():
            for c in range(2):
                move(gain_src.at[0], out.at[0], send_gain.at[c], recv.at[0], c, GAIN_F, waiting)

    all_sends(False)
    all_sends(True)

    for k in range(len(CHUNKS)):
        part = out.at[pl.ds(SLOT0[k], TPD[k])]
        if k == 0:
            @pl.when(me_f != GAIN_F)
            def _():
                pltpu.make_async_copy(part, part, recv.at[k]).wait()

            @pl.when(me_f == GAIN_F)
            def _():
                pltpu.make_async_copy(out.at[0], out.at[0], recv.at[k]).wait()
        else:
            pltpu.make_async_copy(part, part, recv.at[k]).wait()


def spread_tiles(al13, al2, gain_tile):
    return pl.pallas_call(
        spread_kernel,
        out_shape=jax.ShapeDtypeStruct((SLOTS, 8, 1, 128), jnp.float32),
        in_specs=[pl.BlockSpec(memory_space=pltpu.VMEM)] * 3,
        out_specs=pl.BlockSpec(memory_space=pl.ANY),
        scratch_shapes=[
            pltpu.SemaphoreType.DMA((3,)),
            pltpu.SemaphoreType.DMA((15,)),
            pltpu.SemaphoreType.DMA((2,)),
            pltpu.SemaphoreType.DMA((3,)),
        ],
        compiler_params=pltpu.CompilerParams(has_side_effects=True),
        name='spread_tiles',
    )(al13, al2, gain_tile)


def return_kernel(g0, g1, g2, out13, out2, out_gain, send, send_gain, recv13, recv2, recv_gain):
    dev = my_index()
    me_c = lax.axis_index('dp')
    me_f = lax.axis_index('fsdp')

    def all_sends(waiting):
        def send_chunk(k, src):
            n = CHUNKS[k]

            def per_slot(s, carry):
                p = me_f * TPD[k] + s
                row13, col13, row2, col2 = tile_of(k, me_c, p)

                @pl.when(p < 2 * (D // 8) * n)
                def _():
                    owner = (8 * row13) // 21
                    t = row13 - row_start(owner)
                    move(src.at[s], out13.at[pl.ds(t * 8, 8), col13], send.at[k], recv13.at[t], owner // GRP, owner % GRP, waiting)

                @pl.when(p >= 2 * (D // 8) * n)
                def _():
                    owner = FIRST_W2 + (8 * row2 + 38) // 114
                    t = row2 - w2_row_start(owner)
                    move(src.at[s], out2.at[pl.ds(t * 8, 8), col2], send.at[k], recv2.at[t], owner // GRP, owner % GRP, waiting)
                return carry

            lax.fori_loop(0, TPD[k], per_slot, 0)

        send_chunk(2, g2)
        send_chunk(1, g1)

        @pl.when(me_f != GAIN_F)
        def _():
            send_chunk(0, g0)

        @pl.when(me_f == GAIN_F)
        def _():
            move(g0.at[0], out_gain.at[me_c], send_gain, recv_gain.at[me_c], 0, 0, waiting)

    all_sends(False)
    all_sends(True)

    @pl.when(dev < FIRST_W2)
    def _():
        def wait_row(t, carry):
            part = out13.at[pl.ds(t * 8, 8)]
            pltpu.make_async_copy(part, part, recv13.at[t]).wait()
            return carry

        lax.fori_loop(0, row_start(dev + 1) - row_start(dev), wait_row, 0)

    @pl.when(dev >= FIRST_W2)
    def _():
        def wait_row(t, carry):
            part = out2.at[pl.ds(t * 8, 8)]
            pltpu.make_async_copy(part, part, recv2.at[t]).wait()
            return carry

        lax.fori_loop(0, w2_row_start(dev + 1) - w2_row_start(dev), wait_row, 0)

    @pl.when(dev == 0)
    def _():
        for c in range(2):
            pltpu.make_async_copy(out_gain.at[c], out_gain.at[c], recv_gain.at[c]).wait()


def return_tiles(grads):
    tiles = [g.reshape(TPD[k], 8, 1, 128) for k, g in enumerate(grads)]
    return pl.pallas_call(
        return_kernel,
        out_shape=(
            jax.ShapeDtypeStruct((ROWS13, NB, 1, 128), jnp.float32),
            jax.ShapeDtypeStruct((ROWS2, ND, 1, 128), jnp.float32),
            jax.ShapeDtypeStruct((2, 8, 1, 128), jnp.float32),
        ),
        in_specs=[pl.BlockSpec(memory_space=pltpu.VMEM)] * 3,
        out_specs=[pl.BlockSpec(memory_space=pl.ANY)] * 3,
        scratch_shapes=[
            pltpu.SemaphoreType.DMA((3,)),
            pltpu.SemaphoreType.DMA,
            pltpu.SemaphoreType.DMA((3,)),
            pltpu.SemaphoreType.DMA((15,)),
            pltpu.SemaphoreType.DMA((2,)),
        ],
        compiler_params=pltpu.CompilerParams(has_side_effects=True),
        name='return_tiles',
    )(*tiles)


def region_offset(dev):
    first13 = D + 8 * FF * row_start(dev)
    first2 = W2_START + 8 * D * w2_row_start(dev)
    return jnp.where(dev <= FIRST_W2, first13, first2) - SHARD * dev


def chunk_weights(k, tiles):
    n = CHUNKS[k]
    part = (D // 8) * n
    w_one = tiles[:part].reshape(D // 8, n, 8, 128).transpose(0, 2, 1, 3).reshape(D, n * 128)
    w_three = tiles[part:2 * part].reshape(D // 8, n, 8, 128).transpose(0, 2, 1, 3).reshape(D, n * 128)
    w_two = tiles[2 * part:3 * part].reshape(16 * n, ND, 8, 128).transpose(0, 2, 1, 3).reshape(n * 128, D)
    return w_one, w_three, w_two


def chunk_tiles(k, d_one, d_three, d_two, tail):
    n = CHUNKS[k]
    t_one = d_one.reshape(D // 8, 8, n, 128).transpose(0, 2, 1, 3).reshape(-1, 8, 128)
    t_three = d_three.reshape(D // 8, 8, n, 128).transpose(0, 2, 1, 3).reshape(-1, 8, 128)
    t_two = d_two.reshape(16 * n, 8, ND, 128).transpose(0, 2, 1, 3).reshape(-1, 8, 128)
    parts = [t_one, t_three, t_two]
    if tail is not None:
        parts.append(tail)
    return jnp.concatenate(parts, axis=0)


def adam_update(master, adam_m, adam_v, grad_mean):
    m_new = BETA_ONE * adam_m + (1.0 - BETA_ONE) * grad_mean
    v_new = BETA_TWO * adam_v + (1.0 - BETA_TWO) * grad_mean * grad_mean
    m_hat = m_new / (1.0 - BETA_ONE ** ADAM_STEP)
    v_hat = v_new / (1.0 - BETA_TWO ** ADAM_STEP)
    master_new = master - LEARN_RATE * (m_hat / (jnp.sqrt(v_hat) + ADAM_EPS) + DECAY_RATE * master)
    return master_new, m_new, v_new


def dotf(a, b, dims):
    return lax.dot_general(a, b, (dims, ((), ())), preferred_element_type=jnp.float32)


def gather_weights(own):
    dev = my_index()
    ring = [(i, (i - 1) % NDEV) for i in range(NDEV)]
    spill = lax.ppermute(own[:SPILL], ('dp', 'fsdp'), ring)
    start = region_offset(dev)
    longer = jnp.concatenate([own, spill, jnp.zeros((SPILL + AL_LEN - SHARD - SPILL,), jnp.float32)])
    aligned = lax.dynamic_slice(longer, (start,), (AL_LEN,))
    al13 = aligned.reshape(ROWS13, NB, 1, 128)
    al2 = aligned[:ROWS2 * D].reshape(ROWS2, ND, 1, 128)
    gain_tile = own[:1024].reshape(1, 8, 1, 128)
    mine = spread_tiles(al13, al2, gain_tile).reshape(SLOTS, 8, 128).astype(jnp.bfloat16)
    gathered = []
    for k in range(len(CHUNKS)):
        part = mine[SLOT0[k]:SLOT0[k] + TPD[k]].reshape(TPD[k] * 8, 128)
        gathered.append(lax.all_gather(part, 'fsdp', axis=0, tiled=True).reshape(GRP * TPD[k], 8, 128))
    return gathered


def solution(mesh):
    flat_spec = P(None, ('dp', 'fsdp'))
    act_spec = P(None, ('dp', 'fsdp'), None, None)
    swap = [(0, 1), (1, 0)]

    def train_step(master, adam_m, adam_v, inputs, targets):
        token_total = inputs.shape[1] * inputs.shape[2]

        def local_step(master_sh, m_sh, v_sh, x_loc, y_loc):
            dev = my_index()
            tok = x_loc.shape[1] * x_loc.shape[2]
            own = master_sh.reshape(SHARD)
            x_own = x_loc.reshape(tok, D)
            y_own = y_loc.reshape(tok, D)
            gathered = gather_weights(own)
            x_all = jnp.concatenate([x_own, lax.ppermute(x_own, 'dp', swap)], axis=0)
            hidden = x_all.astype(jnp.float32)
            gain_f = gathered[0][GAIN_F * TPD[0]].reshape(1024)[:D].astype(jnp.float32)
            inv_rms = lax.rsqrt(jnp.mean(hidden * hidden, axis=-1, keepdims=True) + RMS_EPS)
            normed_f = hidden * inv_rms
            normed = (normed_f * gain_f).astype(jnp.bfloat16)

            saved = []
            h_part = None
            for k in range(len(CHUNKS)):
                w_one, w_three, w_two = chunk_weights(k, gathered[k])
                gate = dotf(normed, w_one, ((1,), (0,)))
                up = dotf(normed, w_three, ((1,), (0,)))
                inner = (jax.nn.silu(gate) * up).astype(jnp.bfloat16)
                piece = dotf(inner, w_two, ((1,), (0,)))
                h_part = piece if h_part is None else h_part + piece
                saved.append((gate, up, inner, w_one, w_three, w_two))

            other = lax.ppermute(h_part[tok:], 'dp', swap)
            hidden_out = hidden[:tok] + (h_part[:tok] + other)
            err = hidden_out - y_own.astype(jnp.float32)
            loss_sum = 0.5 * jnp.sum(err * err)
            err_b = err.astype(jnp.bfloat16)
            err_all = jnp.concatenate([err_b, lax.ppermute(err_b, 'dp', swap)], axis=0)

            grads = [None] * len(CHUNKS)
            q_sum = None
            for k in reversed(range(len(CHUNKS))):
                gate, up, inner, w_one, w_three, w_two = saved[k]
                sig = jax.nn.sigmoid(gate)
                d_two = dotf(inner, err_all, ((0,), (0,)))
                d_inner = dotf(err_all, w_two, ((1,), (1,)))
                d_gate = (d_inner * up * sig * (1.0 + gate * (1.0 - sig))).astype(jnp.bfloat16)
                d_up = (d_inner * (gate * sig)).astype(jnp.bfloat16)
                d_one = dotf(normed, d_gate, ((0,), (0,)))
                d_three = dotf(normed, d_up, ((0,), (0,)))
                q_k = dotf(d_gate, w_one, ((1,), (1,))) + dotf(d_up, w_three, ((1,), (1,)))
                q_sum = q_k if q_sum is None else q_sum + q_k
                tail = None
                if k == 0:
                    d_gain = jnp.sum(q_sum * normed_f, axis=0)
                    tail = jnp.pad(d_gain, (0, 1024 * TPD[0] - D)).reshape(TPD[0], 8, 128)
                tiles = chunk_tiles(k, d_one, d_three, d_two, tail)
                grads[k] = lax.psum_scatter(tiles.reshape(-1, 128), 'fsdp', scatter_dimension=0, tiled=True)

            loss_value = lax.psum(loss_sum, ('dp', 'fsdp')) / token_total
            out13, out2, out_gain = return_tiles(grads)
            flat13 = out13.reshape(AL_LEN)
            flat2 = jnp.pad(out2.reshape(ROWS2 * D), (0, AL_LEN - ROWS2 * D))
            aligned = jnp.where(dev < FIRST_W2, flat13, flat2)
            start = region_offset(dev)
            longer = jnp.concatenate([jnp.zeros((SPILL,), jnp.float32), aligned, jnp.zeros((SPILL,), jnp.float32)])
            spill = lax.dynamic_slice(longer, (SPILL + SHARD - start,), (SPILL,))
            body = lax.dynamic_slice(longer, (SPILL - start,), (SHARD,))
            ring = [(i, (i + 1) % NDEV) for i in range(NDEV)]
            head = lax.ppermute(spill, ('dp', 'fsdp'), ring)
            gain_grad = (out_gain[0] + out_gain[1]).reshape(1024)
            head = jnp.where(dev == 0, jnp.pad(gain_grad, (0, SPILL - 1024)), head)
            grad_sum = jnp.where(jnp.arange(SHARD) < start, jnp.pad(head, (0, SHARD - SPILL)), body)
            grad_mean = grad_sum.reshape(1, SHARD) / token_total
            master_new, m_new, v_new = adam_update(master_sh, m_sh, v_sh, grad_mean)
            return master_new, m_new, v_new, loss_value

        return jax.shard_map(local_step, mesh=mesh, in_specs=(flat_spec, flat_spec, flat_spec, act_spec, act_spec), out_specs=(flat_spec, flat_spec, flat_spec, P()), check_vma=False)(master, adam_m, adam_v, inputs, targets)

    return train_step
```

```python
import functools

import jax
import jax.numpy as jnp
from jax import lax
from jax.experimental import pallas as pl
from jax.experimental.pallas import tpu as pltpu
from jax.sharding import PartitionSpec as P

ADAM_STEP = 3
LEARN_RATE = 2e-3
BETA_ONE = 0.9
BETA_TWO = 0.999
ADAM_EPS = 1e-8
DECAY_RATE = 0.1
RMS_EPS = 1e-5

D = 896
FF = 4864
FLAT = D * (3 * FF + 1)
NDEV = 128
GRP = 64
SHARD = FLAT // NDEV
NB = FF // 128
ND = D // 128
HB = NB // 2
W2_START = D + 2 * D * FF
FIRST_W2 = 85
SPILL = 35840
ROWS13, ROWS2 = 24, 120
AL_LEN = ROWS13 * FF

MAT = (D // 8) * HB
SLOTS = 100
GAIN_F = GRP - 1
GAIN_SLOT = 3 * MAT - GAIN_F * SLOTS
ROWS = SLOTS * 8
COLOURS = (((0, 144), (144, 128)), ((272, 144), (416, 128)), ((544, 128), (672, 128)))
SUMS = (((0, 17), (17, 17)), ((34, 17), (51, 16)), ((67, 17), (84, 16)))
AXES = ('z', 'y', 'x')

MESH = pl.DeviceIdType.MESH


def row_start(dev):
    return (21 * dev + 7) // 8


def w2_row_start(dev):
    return jnp.maximum((114 * dev - 9728 + 7) // 8, 0)


def my_index():
    return lax.axis_index('dp') * GRP + lax.axis_index('fsdp')


def move(src, dst, send_sem, recv_sem, c, f, waiting):
    stays = (c == lax.axis_index('dp')) & (f == lax.axis_index('fsdp'))

    def remote():
        return pltpu.make_async_remote_copy(
            src_ref=src, dst_ref=dst, send_sem=send_sem, recv_sem=recv_sem, device_id=(c, f), device_id_type=MESH)

    if waiting:
        @pl.when(jnp.logical_not(stays))
        def _():
            remote().wait_send()
    else:
        @pl.when(jnp.logical_not(stays))
        def _():
            remote().start()

        @pl.when(stays)
        def _():
            pltpu.make_async_copy(src, dst, recv_sem).start()


def ring_pos():
    f = lax.axis_index('fsdp')
    return {'z': f // 16, 'y': (f // 4) % 4, 'x': f % 4}


def neighbour(pos, axis, step):
    moved = dict(pos)
    moved[axis] = (pos[axis] + step + 4) % 4
    return (lax.axis_index('dp'), moved['z'] * 16 + moved['y'] * 4 + moved['x'])


def block_set(pos, fixed, rows):
    index = tuple(fixed.get(axis, slice(None)) for axis in AXES)
    return index + (pl.ds(rows[0], rows[1]), slice(None))


def gather_kernel(src13, src2, gain_src, out, land, mine, send13, send2, send_gain, recv_tile, local_sem, send_sem, recv_sem):
    dev = my_index()
    me_f = lax.axis_index('fsdp')
    pos = ring_pos()

    def all_sends(waiting):
        def send(src, c, p, sem):
            move(src, land.at[p % SLOTS], sem, recv_tile, c, p // SLOTS, waiting)

        @pl.when(dev < FIRST_W2)
        def _():
            first = row_start(dev)

            def per_row(t, carry):
                def per_col(j, carry2):
                    for c in range(2):
                        send(src13.at[pl.ds(t * 8, 8), HB * c + j, 0], c, (first + t) * HB + j, send13.at[t])
                    return carry2

                return lax.fori_loop(0, HB, per_col, carry)

            lax.fori_loop(0, row_start(dev + 1) - first, per_row, 0)

        @pl.when(dev >= FIRST_W2)
        def _():
            first = w2_row_start(dev)

            def per_row(t, carry):
                row = first + t
                c = row // (FF // 16)
                base = 2 * MAT + (row % (FF // 16)) * ND

                def per_col(j, carry2):
                    send(src2.at[pl.ds(t * 8, 8), j, 0], c, base + j, send2.at[t])
                    return carry2

                return lax.fori_loop(0, ND, per_col, carry)

            lax.fori_loop(0, w2_row_start(dev + 1) - first, per_row, 0)

        @pl.when(dev == 0)
        def _():
            for c in range(2):
                move(gain_src.at[0, pl.ds(0, 8), 0], land.at[GAIN_SLOT], send_gain.at[c], recv_tile, c, GAIN_F, waiting)

    all_sends(False)
    all_sends(True)

    @pl.when(me_f != GAIN_F)
    def _():
        pltpu.make_async_copy(land, land, recv_tile).wait()

    @pl.when(me_f == GAIN_F)
    def _():
        part = land.at[pl.ds(0, GAIN_SLOT + 1)]
        pltpu.make_async_copy(part, part, recv_tile).wait()

    mine[...] = land[...].reshape(ROWS, 128).astype(jnp.bfloat16)
    own = out.at[pos['z'], pos['y'], pos['x']]
    local = pltpu.make_async_copy(mine, own, local_sem)
    local.start()
    local.wait()

    for phase in range(3):
        def copies(colour, step):
            axis = AXES[(2 - colour - phase) % 3]
            done = [AXES[(2 - colour - q) % 3] for q in range(phase)]
            fixed = {a: pos[a] for a in AXES if a not in done}
            halves = COLOURS[colour]
            both = (halves[0][0], halves[0][1] + halves[1][1])
            made = []
            for way, shift in enumerate((1, -1)):
                where = dict(fixed)
                rows = both
                if step == 1:
                    where[axis] = (pos[axis] - shift + 4) % 4
                    rows = halves[way]
                index = block_set(pos, where, rows)
                made.append(pltpu.make_async_remote_copy(
                    src_ref=out.at[index],
                    dst_ref=out.at[index],
                    send_sem=send_sem.at[colour, phase, step, way],
                    recv_sem=recv_sem.at[colour, phase, step, way],
                    device_id=neighbour(pos, axis, shift),
                    device_id_type=MESH,
                ))
            return made

        for step in range(2):
            for colour in range(3):
                for copy in copies(colour, step):
                    copy.start()
            for colour in range(3):
                for copy in copies(colour, step):
                    copy.wait()


def gather_tiles(al13, al2, gain_tile):
    return pl.pallas_call(
        gather_kernel,
        out_shape=jax.ShapeDtypeStruct((4, 4, 4, ROWS, 128), jnp.bfloat16),
        in_specs=[pl.BlockSpec(memory_space=pltpu.VMEM)] * 3,
        out_specs=pl.BlockSpec(memory_space=pl.ANY),
        scratch_shapes=[
            pltpu.VMEM((SLOTS, 8, 128), jnp.float32),
            pltpu.VMEM((ROWS, 128), jnp.bfloat16),
            pltpu.SemaphoreType.DMA((3,)),
            pltpu.SemaphoreType.DMA((15,)),
            pltpu.SemaphoreType.DMA((2,)),
            pltpu.SemaphoreType.DMA,
            pltpu.SemaphoreType.DMA,
            pltpu.SemaphoreType.DMA((3, 3, 2, 2)),
            pltpu.SemaphoreType.DMA((3, 3, 2, 2)),
        ],
        compiler_params=pltpu.CompilerParams(has_side_effects=True),
        name='gather_tiles',
    )(al13, al2, gain_tile)


def scatter_kernel(g_one, g_three, g_two, g_tail, out13, out2, out_gain, total, relay0, relay1, relay2, merge0, merge1, merge2,
                   load_sem, send_sem, recv_sem, send_tile, send_gain, recv13, recv2, recv_gain):
    dev = my_index()
    me_c = lax.axis_index('dp')
    me_f = lax.axis_index('fsdp')
    pos = ring_pos()
    relays = (relay0, relay1, relay2)
    merges = (merge0, merge1, merge2)

    sources = ((g_one, 0, MAT), (g_three, MAT, 2 * MAT), (g_two, 2 * MAT, 3 * MAT), (g_tail, 3 * MAT, GRP * SLOTS))
    loads = []
    for f in range(GRP):
        for src, low, high in sources:
            first, last = max(low, f * SLOTS), min(high, (f + 1) * SLOTS)
            if first < last:
                dst = total.at[f // 16, (f // 4) % 4, f % 4, pl.ds(first - f * SLOTS, last - first)]
                loads.append(pltpu.make_async_copy(src.at[pl.ds(first - low, last - first)], dst, load_sem.at[len(loads)]))
    for copy in loads:
        copy.start()
    for copy in loads:
        copy.wait()

    for phase in range(3):
        def index_of(colour, at, rows):
            axis = AXES[(colour + phase) % 3]
            done = [AXES[(colour + q) % 3] for q in range(phase)]
            fixed = {a: pos[a] for a in done}
            fixed[axis] = at
            return fixed, rows

        def set_ref(colour, at, rows):
            fixed, rows = index_of(colour, at, rows)
            return total.at[tuple(fixed.get(a, slice(None)) for a in AXES) + (pl.ds(rows[0], rows[1]),)]

        def add_set(colour, at, rows, landed):
            fixed, rows = index_of(colour, at, rows)
            free = [a for a in AXES if a not in fixed]

            def body(i, carry):
                spot = dict(fixed)
                inner = ()
                if len(free) == 2:
                    inner = (i // 4, i % 4)
                elif len(free) == 1:
                    inner = (i,)
                for a, v in zip(free, inner):
                    spot[a] = v
                where = (spot['z'], spot['y'], spot['x'], pl.ds(rows[0], rows[1]))
                value = total[where]
                for part in landed:
                    value = value + part[inner + (pl.ds(0, rows[1]),)]
                total[where] = value
                return carry

            lax.fori_loop(0, 4 ** len(free), body, 0)

        def position(colour):
            return pos[AXES[(colour + phase) % 3]]

        def both(colour):
            halves = SUMS[colour]
            return (halves[0][0], halves[0][1] + halves[1][1])

        def copies(colour, step):
            axis = AXES[(colour + phase) % 3]
            made = []
            for way, shift in enumerate((1, -1)):
                if step == 0:
                    rows = SUMS[colour][way]
                    at = (pos[axis] + 2) % 4
                    dst = relays[phase]
                else:
                    rows = both(colour)
                    at = (pos[axis] + shift + 4) % 4
                    dst = merges[phase]
                lead = (colour, way) + (slice(None),) * (2 - phase)
                made.append(pltpu.make_async_remote_copy(
                    src_ref=set_ref(colour, at, rows),
                    dst_ref=dst.at[lead + (pl.ds(0, rows[1]),)],
                    send_sem=send_sem.at[colour, phase, step, way],
                    recv_sem=recv_sem.at[colour, phase, step, way],
                    device_id=neighbour(pos, axis, shift),
                    device_id_type=MESH,
                ))
            return made

        for colour in range(3):
            for copy in copies(colour, 0):
                copy.start()
        for colour in range(3):
            for copy in copies(colour, 0):
                copy.wait()
            here = position(colour)
            add_set(colour, (here + 1) % 4, SUMS[colour][0], [relays[phase].at[colour, 0]])
            add_set(colour, (here + 3) % 4, SUMS[colour][1], [relays[phase].at[colour, 1]])
            for copy in copies(colour, 1):
                copy.start()
        for colour in range(3):
            for copy in copies(colour, 1):
                copy.wait()
            add_set(colour, position(colour), both(colour), [merges[phase].at[colour, 0], merges[phase].at[colour, 1]])

    mine = total.at[pos['z'], pos['y'], pos['x']]

    def all_sends(waiting):
        def per_slot(s, carry):
            p = me_f * SLOTS + s

            @pl.when(p < 2 * MAT)
            def _():
                row = p // HB
                owner = (8 * row) // 21
                t = row - row_start(owner)
                dst = out13.at[pl.ds(t * 8, 8), HB * me_c + p % HB, 0]
                move(mine.at[s], dst, send_tile, recv13.at[t], owner // GRP, owner % GRP, waiting)

            @pl.when(p >= 2 * MAT)
            def _():
                row = (FF // 16) * me_c + (p - 2 * MAT) // ND
                owner = FIRST_W2 + (8 * row + 38) // 114
                t = row - w2_row_start(owner)
                dst = out2.at[pl.ds(t * 8, 8), (p - 2 * MAT) % ND, 0]
                move(mine.at[s], dst, send_tile, recv2.at[t], owner // GRP, owner % GRP, waiting)
            return carry

        lax.fori_loop(0, jnp.where(me_f == GAIN_F, GAIN_SLOT, SLOTS), per_slot, 0)

        @pl.when(me_f == GAIN_F)
        def _():
            def per_device(d, carry):
                move(mine.at[GAIN_SLOT], out_gain.at[me_c], send_gain, recv_gain.at[me_c], d // GRP, d % GRP, waiting)
                return carry

            lax.fori_loop(0, NDEV, per_device, 0)

    all_sends(False)
    all_sends(True)

    @pl.when(dev < FIRST_W2)
    def _():
        def wait_row(t, carry):
            part = out13.at[pl.ds(t * 8, 8)]
            pltpu.make_async_copy(part, part, recv13.at[t]).wait()
            return carry

        lax.fori_loop(0, row_start(dev + 1) - row_start(dev), wait_row, 0)

    @pl.when(dev >= FIRST_W2)
    def _():
        def wait_row(t, carry):
            part = out2.at[pl.ds(t * 8, 8)]
            pltpu.make_async_copy(part, part, recv2.at[t]).wait()
            return carry

        lax.fori_loop(0, w2_row_start(dev + 1) - w2_row_start(dev), wait_row, 0)

    for c in range(2):
        pltpu.make_async_copy(out_gain.at[c], out_gain.at[c], recv_gain.at[c]).wait()


def scatter_tiles(g_one, g_three, g_two, g_tail):
    half = max(h[1] for pair in SUMS for h in pair)
    full = max(pair[0][1] + pair[1][1] for pair in SUMS)
    relays = [pltpu.VMEM((3, 2) + (4,) * (2 - p) + (half, 8, 128), jnp.float32) for p in range(3)]
    merges = [pltpu.VMEM((3, 2) + (4,) * (2 - p) + (full, 8, 128), jnp.float32) for p in range(3)]
    return pl.pallas_call(
        scatter_kernel,
        out_shape=(
            jax.ShapeDtypeStruct((ROWS13, NB, 1, 128), jnp.float32),
            jax.ShapeDtypeStruct((ROWS2, ND, 1, 128), jnp.float32),
            jax.ShapeDtypeStruct((2, 8, 128), jnp.float32),
        ),
        in_specs=[pl.BlockSpec(memory_space=pl.ANY)] * 4,
        out_specs=[pl.BlockSpec(memory_space=pl.ANY)] * 3,
        scratch_shapes=[
            pltpu.VMEM((4, 4, 4, SLOTS, 8, 128), jnp.float32),
            *relays,
            *merges,
            pltpu.SemaphoreType.DMA((GRP + 3,)),
            pltpu.SemaphoreType.DMA((3, 3, 2, 2)),
            pltpu.SemaphoreType.DMA((3, 3, 2, 2)),
            pltpu.SemaphoreType.DMA,
            pltpu.SemaphoreType.DMA,
            pltpu.SemaphoreType.DMA((3,)),
            pltpu.SemaphoreType.DMA((15,)),
            pltpu.SemaphoreType.DMA((2,)),
        ],
        compiler_params=pltpu.CompilerParams(has_side_effects=True, vmem_limit_bytes=60 * 2 ** 20),
        name='scatter_tiles',
    )(g_one, g_three, g_two, g_tail)


def region_offset(dev):
    first13 = D + 8 * FF * row_start(dev)
    first2 = W2_START + 8 * D * w2_row_start(dev)
    return jnp.where(dev <= FIRST_W2, first13, first2) - SHARD * dev


def as_matrix(tiles, rows, cols):
    return tiles.reshape(rows // 8, cols // 128, 8, 128).transpose(0, 2, 1, 3).reshape(rows, cols)


def as_tiles(matrix):
    rows, cols = matrix.shape
    return matrix.reshape(rows // 8, 8, cols // 128, 128).transpose(0, 2, 1, 3).reshape(-1, 8, 128)


def adam_update(master, adam_m, adam_v, grad_mean):
    m_new = BETA_ONE * adam_m + (1.0 - BETA_ONE) * grad_mean
    v_new = BETA_TWO * adam_v + (1.0 - BETA_TWO) * grad_mean * grad_mean
    m_hat = m_new / (1.0 - BETA_ONE ** ADAM_STEP)
    v_hat = v_new / (1.0 - BETA_TWO ** ADAM_STEP)
    master_new = master - LEARN_RATE * (m_hat / (jnp.sqrt(v_hat) + ADAM_EPS) + DECAY_RATE * master)
    return master_new, m_new, v_new


def dotf(a, b, dims):
    return lax.dot_general(a, b, (dims, ((), ())), preferred_element_type=jnp.float32)


def gather_weights(own):
    dev = my_index()
    ring = [(i, (i - 1) % NDEV) for i in range(NDEV)]
    spill = lax.ppermute(own[:SPILL], ('dp', 'fsdp'), ring)
    start = region_offset(dev)
    longer = jnp.concatenate([own, spill, jnp.zeros((SPILL + AL_LEN - SHARD - SPILL,), jnp.float32)])
    aligned = lax.dynamic_slice(longer, (start,), (AL_LEN,))
    al13 = aligned.reshape(ROWS13, NB, 1, 128)
    al2 = aligned[:ROWS2 * D].reshape(ROWS2, ND, 1, 128)
    gain_tile = own[:1024].reshape(1, 8, 1, 128)
    return gather_tiles(al13, al2, gain_tile).reshape(GRP * SLOTS, 8, 128)


def solution(mesh):
    flat_spec = P(None, ('dp', 'fsdp'))
    act_spec = P(None, ('dp', 'fsdp'), None, None)
    swap = [(0, 1), (1, 0)]

    def train_step(master, adam_m, adam_v, inputs, targets):
        token_total = inputs.shape[1] * inputs.shape[2]

        def local_step(master_sh, m_sh, v_sh, x_loc, y_loc):
            dev = my_index()
            tok = x_loc.shape[1] * x_loc.shape[2]
            own = master_sh.reshape(SHARD)
            x_own = x_loc.reshape(tok, D)
            y_own = y_loc.reshape(tok, D)
            tiles = gather_weights(own)
            w_one = as_matrix(tiles[:MAT], D, HB * 128)
            w_three = as_matrix(tiles[MAT:2 * MAT], D, HB * 128)
            w_two = as_matrix(tiles[2 * MAT:3 * MAT], HB * 128, D)
            gain_f = tiles[GAIN_F * SLOTS + GAIN_SLOT].reshape(1024)[:D].astype(jnp.float32)
            x_all = jnp.concatenate([x_own, lax.ppermute(x_own, 'dp', swap)], axis=0)
            hidden = x_all.astype(jnp.float32)
            inv_rms = lax.rsqrt(jnp.mean(hidden * hidden, axis=-1, keepdims=True) + RMS_EPS)
            normed_f = hidden * inv_rms
            normed = (normed_f * gain_f).astype(jnp.bfloat16)
            gate = dotf(normed, w_one, ((1,), (0,)))
            up = dotf(normed, w_three, ((1,), (0,)))
            inner = (jax.nn.silu(gate) * up).astype(jnp.bfloat16)
            h_part = dotf(inner, w_two, ((1,), (0,)))
            other = lax.ppermute(h_part[tok:], 'dp', swap)
            err = hidden[:tok] + (h_part[:tok] + other) - y_own.astype(jnp.float32)
            loss_sum = 0.5 * jnp.sum(err * err)
            err_b = err.astype(jnp.bfloat16)
            err_all = jnp.concatenate([err_b, lax.ppermute(err_b, 'dp', swap)], axis=0)

            sig = jax.nn.sigmoid(gate)
            d_two = dotf(inner, err_all, ((0,), (0,)))
            d_inner = dotf(err_all, w_two, ((1,), (1,)))
            d_gate = (d_inner * up * sig * (1.0 + gate * (1.0 - sig))).astype(jnp.bfloat16)
            d_up = (d_inner * (gate * sig)).astype(jnp.bfloat16)
            d_one = dotf(normed, d_gate, ((0,), (0,)))
            d_three = dotf(normed, d_up, ((0,), (0,)))
            q_sum = dotf(d_gate, w_one, ((1,), (1,))) + dotf(d_up, w_three, ((1,), (1,)))
            d_gain = jnp.sum(q_sum * normed_f, axis=0)
            tail = jnp.concatenate([d_gain, loss_sum.reshape(1)])
            tail = jnp.pad(tail, (0, 1024 * (SLOTS - GAIN_SLOT) - D - 1)).reshape(SLOTS - GAIN_SLOT, 8, 128)
            out13, out2, out_gain = scatter_tiles(as_tiles(d_one), as_tiles(d_three), as_tiles(d_two), tail)
            sums = (out_gain[0] + out_gain[1]).reshape(1024)
            loss_value = sums[D] / token_total
            flat13 = out13.reshape(AL_LEN)
            flat2 = jnp.pad(out2.reshape(ROWS2 * D), (0, AL_LEN - ROWS2 * D))
            aligned = jnp.where(dev < FIRST_W2, flat13, flat2)
            start = region_offset(dev)
            longer = jnp.concatenate([jnp.zeros((SPILL,), jnp.float32), aligned, jnp.zeros((SPILL,), jnp.float32)])
            spill = lax.dynamic_slice(longer, (SPILL + SHARD - start,), (SPILL,))
            body = lax.dynamic_slice(longer, (SPILL - start,), (SHARD,))
            ring = [(i, (i + 1) % NDEV) for i in range(NDEV)]
            head = lax.ppermute(spill, ('dp', 'fsdp'), ring)
            head = jnp.where(dev == 0, jnp.pad(sums[:D], (0, SPILL - D)), head)
            grad_sum = jnp.where(jnp.arange(SHARD) < start, jnp.pad(head, (0, SHARD - SPILL)), body)
            grad_mean = grad_sum.reshape(1, SHARD) / token_total
            master_new, m_new, v_new = adam_update(master_sh, m_sh, v_sh, grad_mean)
            return master_new, m_new, v_new, loss_value

        return jax.shard_map(local_step, mesh=mesh, in_specs=(flat_spec, flat_spec, flat_spec, act_spec, act_spec), out_specs=(flat_spec, flat_spec, flat_spec, P()), check_vma=False)(master, adam_m, adam_v, inputs, targets)

    return train_step
```

```python
import functools

import jax
import jax.numpy as jnp
from jax import lax
from jax.experimental import pallas as pl
from jax.experimental.pallas import tpu as pltpu
from jax.sharding import PartitionSpec as P

ADAM_STEP = 3
LEARN_RATE = 2e-3
BETA_ONE = 0.9
BETA_TWO = 0.999
ADAM_EPS = 1e-8
DECAY_RATE = 0.1
RMS_EPS = 1e-5

D = 896
FF = 4864
FLAT = D * (3 * FF + 1)
NDEV = 128
GRP = 64
SHARD = FLAT // NDEV
NB = FF // 128
ND = D // 128
LANES = 128
TILE = (8, LANES)
UNIT = (16, LANES)
DT = D // 8
DU = D // 16
FT = FF // 16
HB = NB // 2
W2_START = D + 2 * D * FF
FIRST_W2 = 85
SPILL = 35840
ROWS13, ROWS2 = 24, 120
AL_LEN = ROWS13 * FF

CHUNKS = (3, 4, 4, 4, 4)
OFFS = tuple(sum(CHUNKS[:k]) for k in range(len(CHUNKS)))
CU = (8, 11, 11, 11, 11)
TPD = tuple(2 * u for u in CU)
CSLOT = tuple(sum(TPD[:k]) for k in range(len(CHUNKS)))
CSLOTS = sum(TPD)
UNITS = sum(CU)
COLOURS = range(3)
CCOL = tuple(tuple(int('332443344434443'[3 * k + j]) for j in COLOURS) for k in range(len(CHUNKS)))
COL_LEN = tuple(sum(c[j] for c in CCOL) for j in COLOURS)
COL_BASE = (0, COL_LEN[0], COL_LEN[0] + COL_LEN[1])
TOK_TILE = 512

ORDER = (1, 2, 3, 4, 0)
WAYS = (1, -1)
HOOKS = '035023336311'
DRAIN = '251301261402150316040506'
GAIN_F = GRP - 1
HALF, FULL = 4, 8
AXES = ('z', 'y', 'x')

MESH = pl.DeviceIdType.MESH


def row_start(dev):
    return (21 * dev + 7) // 8


def w2_row_start(dev):
    return jnp.maximum((114 * dev - 9728 + 7) // 8, 0)


def repeat(count, body):
    lax.fori_loop(0, count, body, 0)


def lanes(j):
    return slice(j * LANES, (j + 1) * LANES)


def head(count):
    return pl.ds(0, count)


def eight(t):
    return pl.ds(t * 8, 8)


def my_index():
    return lax.axis_index('dp') * GRP + lax.axis_index('fsdp')


def move(src, dst, send_sem, recv_sem, c, f, waiting):
    stays = (c == lax.axis_index('dp')) & (f == lax.axis_index('fsdp'))

    def remote():
        return pltpu.make_async_remote_copy(
            src_ref=src, dst_ref=dst, send_sem=send_sem, recv_sem=recv_sem, device_id=(c, f), device_id_type=MESH)

    if waiting:
        @pl.when(jnp.logical_not(stays))
        def _():
            remote().wait_send()
    else:
        @pl.when(jnp.logical_not(stays))
        def _():
            remote().start()

        @pl.when(stays)
        def _():
            pltpu.make_async_copy(src, dst, recv_sem).start()


def coords(f):
    return f // 16, (f // 4) % 4, f % 4


def ring_pos():
    f = lax.axis_index('fsdp')
    return dict(zip(AXES, coords(f)))


def neighbour(pos, axis, step):
    moved = dict(pos)
    moved[axis] = (pos[axis] + step + 4) % 4
    return (lax.axis_index('dp'), moved['z'] * 16 + moved['y'] * 4 + moved['x'])


def unit_range(k, colour):
    first = COL_BASE[colour] + sum(c[colour] for c in CCOL[:k])
    inside = sum(CCOL[k][:colour])
    return first, inside, CCOL[k][colour]


def block_set(fixed, first, count):
    return tuple(fixed.get(axis, slice(None)) for axis in AXES) + (pl.ds(first, count),)


def chunk_matrices(units, n):
    flat = units.reshape(-1, *UNIT)
    part = DU * n

    def matrix(low, rows, blocks):
        tiles = flat[low:low + rows * blocks].reshape(rows, blocks, *UNIT)
        return jnp.concatenate([tiles[:, j].reshape(rows * 16, 128) for j in range(blocks)], axis=1)

    return matrix(0, DU, n), matrix(part, DU, n), matrix(2 * part, 8 * n, ND)


def forward_kernel(src13, src2, gain_src, x_own, out, h_out, u_out, t_out, x_out, land, mine, gain_land, x_all, u_all, u_t, h_acc, wbuf,
                   send13, send2, send_gain, recv_tile, recv_gain, x_sem, local_sem, load_sem, save_sem, send_sem, recv_sem):
    dev = my_index()
    me_c = lax.axis_index('dp')
    me_f = lax.axis_index('fsdp')
    pos = ring_pos()
    tok = x_own.shape[0]

    own_x = pltpu.make_async_copy(x_own, x_all.at[pl.ds(0, tok)], x_sem.at[0])
    own_x.start()
    other_x = pltpu.make_async_remote_copy(
        src_ref=x_own, dst_ref=x_all.at[pl.ds(tok, tok)], send_sem=x_sem.at[1], recv_sem=x_sem.at[2],
        device_id=(1 - me_c, me_f), device_id_type=MESH)
    other_x.start()

    def all_sends(waiting):
        def send(src, k, c, p, sem):
            move(src, land.at[CSLOT[k] + p % (TPD[k])], sem, recv_tile.at[k], c, p // (TPD[k]), waiting)

        @pl.when(dev == 0)
        def _():
            def per_device(d, carry):
                move(gain_src.at[0, head(8), 0], gain_land, send_gain, recv_gain, d // GRP, d % GRP, waiting)
                return carry

            repeat(NDEV, per_device)

        @pl.when(dev < FIRST_W2)
        def _():
            first = row_start(dev)

            def per_row(t, carry):
                row = first + t
                for k in range(len(CHUNKS)):
                    n = CHUNKS[k]

                    def per_col(j, carry2):
                        for c in range(2):
                            p = ((row // 2) * n + j) * 2 + row % 2
                            send(src13.at[eight(t), HB * c + OFFS[k] + j, 0], k, c, p, send13.at[t])
                        return carry2

                    repeat(n, per_col)
                return carry

            repeat(row_start(dev + 1) - first, per_row)

        @pl.when(dev >= FIRST_W2)
        def _():
            first = w2_row_start(dev)

            def per_row(t, carry):
                row = first + t
                c = row // FT
                kk = row % FT
                for k in range(len(CHUNKS)):
                    n = CHUNKS[k]

                    @pl.when((kk >= 16 * OFFS[k]) & (kk < 16 * (OFFS[k] + n)))
                    def _():
                        local = kk - 16 * OFFS[k]

                        def per_col(j, carry2):
                            p = 2 * DT * n + ((local // 2) * ND + j) * 2 + local % 2
                            send(src2.at[eight(t), j, 0], k, c, p, send2.at[t])
                            return carry2

                        repeat(ND, per_col)
                return carry

            repeat(w2_row_start(dev + 1) - first, per_row)

    all_sends(False)
    all_sends(True)

    for k in range(len(CHUNKS)):
        tiles = 3 * DT * CHUNKS[k]
        whole, rest = tiles // (TPD[k]), tiles % (TPD[k])

        @pl.when(me_f < whole)
        def _():
            part = land.at[pl.ds(CSLOT[k], TPD[k])]
            pltpu.make_async_copy(part, part, recv_tile.at[k]).wait()

        if rest:
            @pl.when(me_f == whole)
            def _():
                part = land.at[pl.ds(CSLOT[k], rest)]
                pltpu.make_async_copy(part, part, recv_tile.at[k]).wait()
        for colour in COLOURS:
            first, inside, count = unit_range(k, colour)
            value = land[CSLOT[k] + 2 * inside:CSLOT[k] + 2 * (inside + count)]
            mine[first:first + count] = value.reshape(count, *UNIT).astype(jnp.bfloat16)
    local = pltpu.make_async_copy(mine, out.at[pos['z'], pos['y'], pos['x']], local_sem)
    local.start()
    local.wait()

    def axis_of(colour, phase):
        return AXES[(2 - colour - phase) % 3]

    def ring_copies(colour, phase, step, first, count, sem):
        axis = axis_of(colour, phase)
        done = [axis_of(colour, q) for q in range(phase)]
        made = []
        for way, shift in enumerate(WAYS):
            where = {a: pos[a] for a in AXES if a not in done}
            low, size = first, count
            if step == 1:
                where[axis] = (pos[axis] - shift + 4) % 4
                size = (count + 1) // 2 if way == 0 else count // 2
                low = first if way == 0 else first + (count + 1) // 2
            index = block_set(where, low, size)
            made.append(pltpu.make_async_remote_copy(
                src_ref=out.at[index],
                dst_ref=out.at[index],
                send_sem=send_sem.at[sem, step, way],
                recv_sem=recv_sem.at[sem, step, way],
                device_id=neighbour(pos, axis, shift),
                device_id_type=MESH,
            ))
        return made

    def start_all(copies):
        for copy in copies:
            copy.start()

    def wait_all(copies):
        for copy in copies:
            copy.wait()

    def early(phase, step):
        return [c for j in COLOURS for c in ring_copies(j, phase, step, COL_BASE[j], COL_LEN[j], phase * 3 + j)]

    def late(k, step):
        made = []
        for j in COLOURS:
            first, _, count = unit_range(k, j)
            made += ring_copies(j, 2, step, first, count, 6 + k * 3 + j)
        return made

    start_all(early(0, 0))
    pltpu.make_async_copy(gain_land, gain_land, recv_gain).wait()
    own_x.wait()
    other_x.wait()
    gain = jnp.concatenate([gain_land[i:i + 1, :] for i in range(ND)], axis=1).astype(jnp.bfloat16).astype(jnp.float32)

    def normalise(t, carry):
        rows = pl.ds(pl.multiple_of(t * 256, 256), 256)
        hidden = x_all[rows, :].astype(jnp.float32)
        inv_rms = lax.rsqrt(jnp.mean(hidden * hidden, axis=-1, keepdims=True) + RMS_EPS)
        normed = hidden * inv_rms * gain
        u_all[rows, :] = normed.astype(jnp.bfloat16)
        u_t[:, rows] = normed.T.astype(jnp.bfloat16)
        return carry

    half_tiles = x_all.shape[0] // 512
    repeat(half_tiles, normalise)
    wait_all(early(0, 0))
    start_all(early(0, 1))
    lax.fori_loop(half_tiles, 2 * half_tiles, normalise, 0)
    wait_all(early(0, 1))
    start_all(early(1, 0))
    u_save = pltpu.make_async_copy(u_all, u_out, save_sem.at[0])
    x_save = pltpu.make_async_copy(x_all, x_out, save_sem.at[1])
    t_save = pltpu.make_async_copy(u_t, t_out, save_sem.at[3])
    u_save.start()
    x_save.start()
    t_save.start()
    wait_all(early(1, 0))
    start_all(early(1, 1))
    wait_all(early(1, 1))

    def loads(k):
        made = []
        for j in COLOURS:
            first, inside, count = unit_range(k, j)
            made.append(pltpu.make_async_copy(
                out.at[:, :, :, pl.ds(first, count)], wbuf.at[k % 2, :, :, :, pl.ds(inside, count)], load_sem.at[k % 2, j]))
        return made

    def compute(k):
        n = CHUNKS[k]

        def tile(t, carry):
            rows = pl.ds(pl.multiple_of(t * TOK_TILE, TOK_TILE), TOK_TILE)
            w_one, w_three, w_two = chunk_matrices(wbuf[k % 2, :, :, :, 0:CU[k]], n)
            u = u_all[rows, :]
            gate = jnp.dot(u, w_one, preferred_element_type=jnp.float32)
            up = jnp.dot(u, w_three, preferred_element_type=jnp.float32)
            inner = (gate * jax.nn.sigmoid(gate) * up).astype(jnp.bfloat16)
            piece = jnp.dot(inner, w_two, preferred_element_type=jnp.float32)
            h_acc[rows, :] = piece if k == 0 else h_acc[rows, :] + piece
            return carry

        repeat(x_all.shape[0] // TOK_TILE, tile)

    last = len(CHUNKS) - 1
    start_all(late(0, 0))
    start_all(late(1, 0))
    for k in range(last + 1):
        wait_all(late(k, 0))
        start_all(late(k, 1))
        if k + 2 <= last:
            start_all(late(k + 2, 0))
        if k >= 1:
            wait_all(loads(k - 1))
            compute(k - 1)
        wait_all(late(k, 1))
        start_all(loads(k))
    wait_all(loads(last))
    compute(last)
    h_save = pltpu.make_async_copy(h_acc, h_out, save_sem.at[2])
    h_save.start()
    h_save.wait()
    u_save.wait()
    x_save.wait()
    t_save.wait()


def forward_tiles(al13, al2, gain_tile, x_own):
    tok = 2 * x_own.shape[0]
    return pl.pallas_call(
        forward_kernel,
        out_shape=(
            jax.ShapeDtypeStruct((4, 4, 4, UNITS, *UNIT), jnp.bfloat16),
            jax.ShapeDtypeStruct((tok, D), jnp.float32),
            jax.ShapeDtypeStruct((tok, D), jnp.bfloat16),
            jax.ShapeDtypeStruct((D, tok), jnp.bfloat16),
            jax.ShapeDtypeStruct((tok, D), jnp.bfloat16),
        ),
        in_specs=[pl.BlockSpec(memory_space=pltpu.VMEM)] * 3 + [pl.BlockSpec(memory_space=pl.ANY)],
        out_specs=[pl.BlockSpec(memory_space=pl.ANY)] * 5,
        scratch_shapes=[
            pltpu.VMEM((CSLOTS, *TILE), jnp.float32),
            pltpu.VMEM((UNITS, *UNIT), jnp.bfloat16),
            pltpu.VMEM(TILE, jnp.float32),
            pltpu.VMEM((tok, D), jnp.bfloat16),
            pltpu.VMEM((tok, D), jnp.bfloat16),
            pltpu.VMEM((D, tok), jnp.bfloat16),
            pltpu.VMEM((tok, D), jnp.float32),
            pltpu.VMEM((2, 4, 4, 4, max(CU), *UNIT), jnp.bfloat16),
            pltpu.SemaphoreType.DMA((3,)),
            pltpu.SemaphoreType.DMA((15,)),
            pltpu.SemaphoreType.DMA,
            pltpu.SemaphoreType.DMA((len(CHUNKS),)),
            pltpu.SemaphoreType.DMA,
            pltpu.SemaphoreType.DMA((3,)),
            pltpu.SemaphoreType.DMA,
            pltpu.SemaphoreType.DMA((2, 3)),
            pltpu.SemaphoreType.DMA((4,)),
            pltpu.SemaphoreType.DMA((6 + 3 * len(CHUNKS), 2, 2)),
            pltpu.SemaphoreType.DMA((6 + 3 * len(CHUNKS), 2, 2)),
        ],
        compiler_params=pltpu.CompilerParams(has_side_effects=True, vmem_limit_bytes=60 * 2 ** 20),
        name='forward_tiles',
    )(al13, al2, gain_tile, x_own)


def cut_tiles(count):
    sizes = [(count + 2 - j) // 3 for j in COLOURS]
    return tuple((sum(sizes[:j]), sizes[j]) for j in COLOURS)


def nt(a, b):
    return lax.dot_general(a, b, (((1,), (1,)), ((), ())), preferred_element_type=jnp.float32)


def backward_kernel(units, u_hbm, t_hbm, x_hbm, e_hbm, loss_tile, out13, out2, out_gain,
                    total, relay0, relay1, relay2, merge0, merge1, merge2, ring_sum, final, wbuf, u_all, u_t, x_all, e_all, r_all,
                    d_gate, d_up, inner, gain_acc,
                    load_sem, w_sem, send_sem, recv_sem, send_tile, send_gain, recv13, recv2, recv_gain, credit, credit_late):
    dev = my_index()
    me_c = lax.axis_index('dp')
    me_f = lax.axis_index('fsdp')
    pos = ring_pos()
    relays = (relay0, relay1, relay2)
    merges = (merge0, merge1, merge2)
    tok = u_all.shape[0]

    def weight_loads(i):
        k = ORDER[i]
        made = []
        for j in COLOURS:
            first, inside, count = unit_range(k, j)
            made.append(pltpu.make_async_copy(
                units.at[:, :, :, pl.ds(first, count)], wbuf.at[i % 2, :, :, :, pl.ds(inside, count)], w_sem.at[i % 2, j]))
        return made

    def start_all(copies):
        for copy in copies:
            copy.start()

    def wait_all(copies):
        for copy in copies:
            copy.wait()

    inputs = [pltpu.make_async_copy(src, dst, load_sem.at[i])
              for i, (src, dst) in enumerate(((u_hbm, u_all), (e_hbm, e_all), (x_hbm, x_all), (t_hbm, u_t)))]
    start_all(weight_loads(0))
    start_all(inputs)

    def axis_of(colour, phase):
        return AXES[(colour + phase) % 3]

    def set_ref(i, colour, phase, at, rows):
        first = axis_of(colour, 0)
        tiles = (pl.ds(*rows),)
        if phase == 0:
            return total.at[(i % 2,) + tuple(at if a == first else slice(None) for a in AXES) + tiles]
        fixed = {axis_of(colour, q): pos[axis_of(colour, q)] for q in range(phase)}
        fixed[axis_of(colour, phase)] = at
        spot = tuple(fixed.get(a, slice(None)) for a in AXES if a != first)
        return ring_sum.at[(i % 3, colour) + spot + (pl.ds(rows[0] - cut_tiles(TPD[ORDER[i]])[colour][0], rows[1]),)]

    def rows_of(i, colour, way):
        first, size = cut_tiles(TPD[ORDER[i]])[colour]
        half = (size + 1) // 2
        return ((first, half), (first + half, size - half), (first, size))[way]

    def copies(i, colour, phase, step):
        axis = axis_of(colour, phase)
        made = []
        for way, shift in enumerate(WAYS):
            rows = rows_of(i, colour, way if step == 0 else 2)
            at = (pos[axis] + (2 if step == 0 else shift + 4)) % 4
            dst = (relays if step == 0 else merges)[phase]
            lead = (i % 2, colour, way) + (slice(None),) * (2 - phase)
            sem = (i % 2, colour * 3 + phase, step, way)
            made.append(pltpu.make_async_remote_copy(
                src_ref=set_ref(i, colour, phase, at, rows),
                dst_ref=dst.at[lead + (head(rows[1]),)],
                send_sem=send_sem.at[sem],
                recv_sem=recv_sem.at[sem],
                device_id=neighbour(pos, axis, shift),
                device_id_type=MESH,
            ))
        return made

    def add_set(i, colour, phase, at, rows, landed, done):
        src = set_ref(i, colour, phase, at, rows)

        def body(b, carry):
            spot = ((b // 4, b % 4), (b,), ())[phase]
            value = src[spot + (slice(None),)]
            for part in landed:
                value = value + part[spot + (head(rows[1]),)]
            if not done or phase == 1:
                src[spot + (slice(None),)] = value
            elif phase == 0:
                ring_sum[(i % 3, colour) + spot + (head(rows[1]),)] = value
            else:
                final[i, pl.ds(*rows)] = value
            return carry

        repeat(4 ** (2 - phase), body)

    def tell_neighbours(sem):
        for axis in AXES:
            for shift in WAYS:
                pl.semaphore_signal(sem, inc=1, device_id=neighbour(pos, axis, shift), device_id_type=MESH)

    def reduce_step(i, s):
        if s == 2 and i >= 2:
            pl.semaphore_wait(credit_late.at[i - 2], 6)
        for colour in COLOURS:
            if s > 0:
                phase, step = (s - 1) // 2, (s - 1) % 2
                here = pos[axis_of(colour, phase)]
                wait_all(copies(i, colour, phase, step))
                if step == 0:
                    for way, shift in enumerate((1, 3)):
                        add_set(i, colour, phase, (here + shift) % 4, rows_of(i, colour, way), [relays[phase].at[i % 2, colour, way]], False)
                else:
                    add_set(i, colour, phase, here, rows_of(i, colour, 2),
                            [merges[phase].at[i % 2, colour, way] for way in range(2)], True)
            if s < 6:
                start_all(copies(i, colour, s // 2, s % 2))
        if i + 2 < len(ORDER):
            if s == 2:
                tell_neighbours(credit.at[i])
            elif s == 6:
                tell_neighbours(credit_late.at[i])
        if s == 6:
            send_home(i, False)

    def send_home(i, waiting):
        k = ORDER[i]
        n = CHUNKS[k]
        own = TPD[k]

        def per_slot(slot, carry):
            p = me_f * own + slot

            @pl.when(p < 2 * DT * n)
            def _():
                q = p // 2
                row = (q // n) * 2 + p % 2
                owner = (8 * row) // 21
                t = row - row_start(owner)
                dst = out13.at[eight(t), HB * me_c + OFFS[k] + q % n, 0]
                move(final.at[i, slot], dst, send_tile.at[i], recv13.at[t], owner // GRP, owner % GRP, waiting)

            @pl.when(p >= 2 * DT * n)
            def _():
                q = (p - 2 * DT * n) // 2
                row = FT * me_c + 16 * OFFS[k] + (q // ND) * 2 + p % 2
                owner = FIRST_W2 + (8 * row + 38) // 114
                t = row - w2_row_start(owner)
                dst = out2.at[eight(t), q % ND, 0]
                move(final.at[i, slot], dst, send_tile.at[i], recv2.at[t], owner // GRP, owner % GRP, waiting)
            return carry

        repeat(jnp.clip(3 * DT * n - me_f * own, 0, own), per_slot)
        if k == 0:
            @pl.when(me_f == GAIN_F)
            def _():
                def per_device(d, carry):
                    move(final.at[i, 0], out_gain.at[me_c], send_gain, recv_gain.at[me_c], d // GRP, d % GRP, waiting)
                    return carry

                repeat(NDEV, per_device)

    def store_tiles(i, first, value):
        own = CU[ORDER[i]]
        count = value.shape[0]
        for f in range(first // own, (first + count + own - 1) // own):
            low, high = max(first, f * own), min(first + count, (f + 1) * own)
            part = value[low - first:high - first].reshape((high - low) * 2, *TILE)
            z, y, x = coords(f)
            total[i % 2, z, y, x, pl.ds((low - f * own) * 2, (high - low) * 2)] = part

    def to_units(matrix):
        blocks = matrix.shape[1] // 128
        cols = [matrix[:, lanes(j)].reshape(-1, 1, *UNIT) for j in range(blocks)]
        return jnp.concatenate(cols, axis=1).reshape(-1, *UNIT)

    def token_tile(i, t, hooks):
        n = CHUNKS[ORDER[i]]
        width = LANES * n
        rows = pl.ds(pl.multiple_of(t * TOK_TILE, TOK_TILE), TOK_TILE)
        w_one, w_three, w_two = chunk_matrices(wbuf[i % 2, :, :, :, 0:CU[ORDER[i]]], n)
        u = u_all[rows, :]
        gate = jnp.dot(u, w_one, preferred_element_type=jnp.float32)
        up = jnp.dot(u, w_three, preferred_element_type=jnp.float32)
        d_inner = nt(e_all[rows, :], w_two)
        sig = jax.nn.sigmoid(gate)
        silu = gate * sig
        inner[rows, 0:width] = (silu * up).astype(jnp.bfloat16)
        dg = (d_inner * up * sig * (1.0 + gate * (1.0 - sig))).astype(jnp.bfloat16)
        du = (d_inner * silu).astype(jnp.bfloat16)
        d_gate[rows, 0:width] = dg
        d_up[rows, 0:width] = du
        q = nt(dg, w_one) + nt(du, w_three)
        x = x_all[rows, :].astype(jnp.float32)
        if i == 0:
            r_all[rows, :] = lax.rsqrt(jnp.mean(x * x, axis=-1, keepdims=True) + RMS_EPS)
        piece = (q * (x * r_all[rows, :])).reshape(TOK_TILE // 8, 8, D)
        gain_acc[...] += jnp.sum(piece, axis=0)
        for at, hook in hooks:
            pl.when(t == at)(hook)

    gain_acc[...] = jnp.zeros_like(gain_acc)
    wait_all(inputs)
    for i in range(len(ORDER)):
        k = ORDER[i]
        n = CHUNKS[k]
        width = LANES * n
        wait_all(weight_loads(i))
        if i + 1 < len(ORDER):
            start_all(weight_loads(i + 1))
        plan = [tuple(map(int, HOOKS[at:at + 3])) for at in range(0, len(HOOKS), 3)]
        hooks = [(at, functools.partial(reduce_step, i - back, s)) for at, back, s in plan if i >= back]

        def tile(t, carry, i=i, hooks=hooks):
            token_tile(i, t, hooks)
            return carry

        repeat(tok // TOK_TILE, tile)
        store_tiles(i, 0, to_units(jnp.dot(u_t[...], d_gate[:, 0:width], preferred_element_type=jnp.float32)))
        store_tiles(i, DU * n, to_units(jnp.dot(u_t[...], d_up[:, 0:width], preferred_element_type=jnp.float32)))
        d_two = lax.dot_general(inner[:, 0:width], e_all[...], (((0,), (0,)), ((), ())), preferred_element_type=jnp.float32)
        store_tiles(i, 2 * DU * n, to_units(d_two))
        if k == 0:
            d_gain = jnp.sum(gain_acc[...], axis=0, keepdims=True)
            rows = [d_gain[:, lanes(j)] for j in range(ND)]
            total[i % 2, 3, 3, 3, 0] = jnp.concatenate(rows + [loss_tile[7:8, :]], axis=0)
        if i >= 2:
            reduce_step(i - 2, 4)
        if i >= 1:
            reduce_step(i - 1, 2)
        if i >= 2:
            pl.semaphore_wait(credit.at[i - 2], 6)
        reduce_step(i, 0)

    last = len(ORDER) - 1
    for back, s in zip(DRAIN[::2], DRAIN[1::2]):
        reduce_step(last - int(back), int(s))
    for i in range(len(ORDER)):
        send_home(i, True)

    @pl.when(dev < FIRST_W2)
    def _():
        def wait_row(t, carry):
            part = out13.at[eight(t)]
            pltpu.make_async_copy(part, part, recv13.at[t]).wait()
            return carry

        repeat(row_start(dev + 1) - row_start(dev), wait_row)

    @pl.when(dev >= FIRST_W2)
    def _():
        def wait_row(t, carry):
            part = out2.at[eight(t)]
            pltpu.make_async_copy(part, part, recv2.at[t]).wait()
            return carry

        repeat(w2_row_start(dev + 1) - w2_row_start(dev), wait_row)

    for c in range(2):
        pltpu.make_async_copy(out_gain.at[c], out_gain.at[c], recv_gain.at[c]).wait()


def backward_tiles(units, u, u_t, x, err, loss_tile):
    tok = u.shape[0]
    width = 128 * max(CHUNKS)
    relays = [pltpu.VMEM((2, 3, 2) + (4,) * (2 - p) + (HALF, *TILE), jnp.float32) for p in COLOURS]
    merges = [pltpu.VMEM((2, 3, 2) + (4,) * (2 - p) + (FULL, *TILE), jnp.float32) for p in COLOURS]
    bf16_act = pltpu.VMEM((tok, D), jnp.bfloat16)
    chunk_act = pltpu.VMEM((tok, width), jnp.bfloat16)
    dma = pltpu.SemaphoreType.DMA
    return pl.pallas_call(
        backward_kernel,
        out_shape=(
            jax.ShapeDtypeStruct((ROWS13, NB, 1, LANES), jnp.float32),
            jax.ShapeDtypeStruct((ROWS2, ND, 1, LANES), jnp.float32),
            jax.ShapeDtypeStruct((2, *TILE), jnp.float32),
        ),
        in_specs=[pl.BlockSpec(memory_space=pl.ANY)] * 5 + [pl.BlockSpec(memory_space=pltpu.VMEM)],
        out_specs=[pl.BlockSpec(memory_space=pl.ANY)] * 3,
        scratch_shapes=[
            pltpu.VMEM((2, 4, 4, 4, max(TPD), *TILE), jnp.float32),
            *relays,
            *merges,
            pltpu.VMEM((3, 3, 4, 4, FULL, *TILE), jnp.float32),
            pltpu.VMEM((len(ORDER), max(TPD), *TILE), jnp.float32),
            pltpu.VMEM((2, 4, 4, 4, max(CU), *UNIT), jnp.bfloat16),
            bf16_act,
            pltpu.VMEM((D, tok), jnp.bfloat16),
            bf16_act,
            bf16_act,
            pltpu.VMEM((tok, 1), jnp.float32),
            chunk_act,
            chunk_act,
            chunk_act,
            pltpu.VMEM((8, D), jnp.float32),
            dma((4,)),
            dma((2, 3)),
            dma((2, 9, 2, 2)),
            dma((2, 9, 2, 2)),
            dma((len(ORDER),)),
            dma,
            dma((3,)),
            dma((15,)),
            dma((2,)),
            pltpu.SemaphoreType.REGULAR((len(ORDER),)),
            pltpu.SemaphoreType.REGULAR((len(ORDER),)),
        ],
        compiler_params=pltpu.CompilerParams(has_side_effects=True, vmem_limit_bytes=63 * 2 ** 20),
        name='backward_tiles',
    )(units, u, u_t, x, err, loss_tile)


def region_offset(dev):
    first13 = D + 8 * FF * row_start(dev)
    first2 = W2_START + 8 * D * w2_row_start(dev)
    return jnp.where(dev <= FIRST_W2, first13, first2) - SHARD * dev


def adam_update(master, adam_m, adam_v, grad_mean):
    m_new = BETA_ONE * adam_m + (1.0 - BETA_ONE) * grad_mean
    v_new = BETA_TWO * adam_v + (1.0 - BETA_TWO) * grad_mean * grad_mean
    m_hat = m_new / (1.0 - BETA_ONE ** ADAM_STEP)
    v_hat = v_new / (1.0 - BETA_TWO ** ADAM_STEP)
    master_new = master - LEARN_RATE * (m_hat / (jnp.sqrt(v_hat) + ADAM_EPS) + DECAY_RATE * master)
    return master_new, m_new, v_new


def aligned_region(own):
    dev = my_index()
    ring = [(i, (i - 1) % NDEV) for i in range(NDEV)]
    spill = lax.ppermute(own[:SPILL], ('dp', 'fsdp'), ring)
    start = region_offset(dev)
    longer = jnp.concatenate([own, spill, jnp.zeros((SPILL + AL_LEN - SHARD - SPILL,), jnp.float32)])
    aligned = lax.dynamic_slice(longer, (start,), (AL_LEN,))
    al13 = aligned.reshape(ROWS13, NB, 1, LANES)
    al2 = aligned[:ROWS2 * D].reshape(ROWS2, ND, 1, LANES)
    gain_tile = own[:1024].reshape(1, 8, 1, LANES)
    return al13, al2, gain_tile


def solution(mesh):
    flat_spec = P(None, ('dp', 'fsdp'))
    act_spec = P(None, ('dp', 'fsdp'), None, None)
    swap = [(0, 1), (1, 0)]

    def train_step(master, adam_m, adam_v, inputs, targets):
        token_total = inputs.shape[1] * inputs.shape[2]

        def local_step(master_sh, m_sh, v_sh, x_loc, y_loc):
            dev = my_index()
            tok = x_loc.shape[1] * x_loc.shape[2]
            own = master_sh.reshape(SHARD)
            x_own = x_loc.reshape(tok, D)
            y_own = y_loc.reshape(tok, D)
            al13, al2, gain_tile = aligned_region(own)
            units, h_part, normed, normed_t, x_all = forward_tiles(al13, al2, gain_tile, x_own)
            other = lax.ppermute(h_part[tok:], 'dp', swap)
            err = x_own.astype(jnp.float32) + (h_part[:tok] + other) - y_own.astype(jnp.float32)
            loss_sum = 0.5 * jnp.sum(err * err)
            err_b = err.astype(jnp.bfloat16)
            err_all = jnp.concatenate([err_b, lax.ppermute(err_b, 'dp', swap)], axis=0)

            loss_tile = jnp.pad(loss_sum.reshape(1), (D, 127)).reshape(TILE)
            out13, out2, out_gain = backward_tiles(units, normed, normed_t, x_all, err_all, loss_tile)
            sums = (out_gain[0] + out_gain[1]).reshape(1024)
            loss_value = sums[D] / token_total
            flat13 = out13.reshape(AL_LEN)
            flat2 = jnp.pad(out2.reshape(ROWS2 * D), (0, AL_LEN - ROWS2 * D))
            aligned = jnp.where(dev < FIRST_W2, flat13, flat2)
            start = region_offset(dev)
            longer = jnp.concatenate([jnp.zeros((SPILL,), jnp.float32), aligned, jnp.zeros((SPILL,), jnp.float32)])
            spill = lax.dynamic_slice(longer, (SPILL + SHARD - start,), (SPILL,))
            body = lax.dynamic_slice(longer, (SPILL - start,), (SHARD,))
            ring = [(i, (i + 1) % NDEV) for i in range(NDEV)]
            head = lax.ppermute(spill, ('dp', 'fsdp'), ring)
            head = jnp.where(dev == 0, jnp.pad(sums[:D], (0, SPILL - D)), head)
            grad_sum = jnp.where(jnp.arange(SHARD) < start, jnp.pad(head, (0, SHARD - SPILL)), body)
            grad_mean = grad_sum.reshape(1, SHARD) / token_total
            master_new, m_new, v_new = adam_update(master_sh, m_sh, v_sh, grad_mean)
            return master_new, m_new, v_new, loss_value

        return jax.shard_map(local_step, mesh=mesh, in_specs=(flat_spec, flat_spec, flat_spec, act_spec, act_spec), out_specs=(flat_spec, flat_spec, flat_spec, P()), check_vma=False)(master, adam_m, adam_v, inputs, targets)

    return train_step
```

```python
import functools

import jax
import jax.numpy as jnp
from jax import lax
from jax.experimental import pallas as pl
from jax.experimental.pallas import tpu as pltpu
from jax.sharding import PartitionSpec as P

ADAM_STEP = 3
LEARN_RATE = 2e-3
BETA_ONE = 0.9
BETA_TWO = 0.999
ADAM_EPS = 1e-8
DECAY_RATE = 0.1
RMS_EPS = 1e-5

D = 896
FF = 4864
FLAT = D * (3 * FF + 1)
NDEV = 128
GRP = 64
SHARD = FLAT // NDEV
NB = FF // 128
ND = D // 128
LANES = 128
TILE = (8, LANES)
UNIT = (16, LANES)
DT = D // 8
DU = D // 16
FT = FF // 16
HB = NB // 2
W2_START = D + 2 * D * FF
FIRST_W2 = 85
SPILL = 35840
ROWS13, ROWS2 = 24, 120
AL_LEN = ROWS13 * FF

CHUNKS = (3, 4, 4, 4, 4)
OFFS = tuple(sum(CHUNKS[:k]) for k in range(len(CHUNKS)))
CU = (8, 11, 11, 11, 11)
TPD = tuple(2 * u for u in CU)
CSLOT = tuple(sum(TPD[:k]) for k in range(len(CHUNKS)))
CSLOTS = sum(TPD)
UNITS = sum(CU)
COLOURS = range(3)
CCOL = tuple(tuple(int('332443344434443'[3 * k + j]) for j in COLOURS) for k in range(len(CHUNKS)))
COL_LEN = tuple(sum(c[j] for c in CCOL) for j in COLOURS)
COL_BASE = (0, COL_LEN[0], COL_LEN[0] + COL_LEN[1])
TOK_TILE = 512

ORDER = (1, 2, 3, 4, 0)
WAYS = (1, -1)
HOOKS = '046122234211323335'
DRAIN = '361224011325261402150316040506'
GAIN_F = GRP - 1
HALF, FULL = 4, 8
AXES = ('z', 'y', 'x')

MESH = pl.DeviceIdType.MESH


def row_start(dev):
    return (21 * dev + 7) // 8


def w2_row_start(dev):
    return jnp.maximum((114 * dev - 9728 + 7) // 8, 0)


def repeat(count, body):
    lax.fori_loop(0, count, body, 0)


def lanes(j):
    return slice(j * LANES, (j + 1) * LANES)


def head(count):
    return pl.ds(0, count)


def eight(t):
    return pl.ds(t * 8, 8)


def my_index():
    return lax.axis_index('dp') * GRP + lax.axis_index('fsdp')


def move(src, dst, send_sem, recv_sem, c, f, waiting):
    stays = (c == lax.axis_index('dp')) & (f == lax.axis_index('fsdp'))

    def remote():
        return pltpu.make_async_remote_copy(
            src_ref=src, dst_ref=dst, send_sem=send_sem, recv_sem=recv_sem, device_id=(c, f), device_id_type=MESH)

    if waiting:
        @pl.when(jnp.logical_not(stays))
        def _():
            remote().wait_send()
    else:
        @pl.when(jnp.logical_not(stays))
        def _():
            remote().start()

        @pl.when(stays)
        def _():
            pltpu.make_async_copy(src, dst, recv_sem).start()


def coords(f):
    return f // 16, (f // 4) % 4, f % 4


def ring_pos():
    f = lax.axis_index('fsdp')
    return dict(zip(AXES, coords(f)))


def neighbour(pos, axis, step):
    moved = dict(pos)
    moved[axis] = (pos[axis] + step + 4) % 4
    return (lax.axis_index('dp'), moved['z'] * 16 + moved['y'] * 4 + moved['x'])


def unit_range(k, colour):
    first = COL_BASE[colour] + sum(c[colour] for c in CCOL[:k])
    inside = sum(CCOL[k][:colour])
    return first, inside, CCOL[k][colour]


def block_set(fixed, first, count):
    return tuple(fixed.get(axis, slice(None)) for axis in AXES) + (pl.ds(first, count),)


def chunk_matrices(units, n):
    flat = units.reshape(-1, *UNIT)
    part = DU * n

    def matrix(low, rows, blocks):
        tiles = flat[low:low + rows * blocks].reshape(rows, blocks, *UNIT)
        return jnp.concatenate([tiles[:, j].reshape(rows * 16, 128) for j in range(blocks)], axis=1)

    return matrix(0, DU, n), matrix(part, DU, n), matrix(2 * part, 8 * n, ND)


def forward_kernel(src13, src2, gain_src, x_own, out, h_mine, h_other, u_out, t_out, x_out, land, mine, gain_land, x_all, u_all, u_t, h_acc, wbuf,
                   send13, send2, send_gain, recv_tile, recv_gain, x_sem, local_sem, load_sem, save_sem, h_sem, send_sem, recv_sem):
    dev = my_index()
    me_c = lax.axis_index('dp')
    me_f = lax.axis_index('fsdp')
    pos = ring_pos()
    tok = x_own.shape[0]

    own_x = pltpu.make_async_copy(x_own, x_all.at[pl.ds(0, tok)], x_sem.at[0])
    own_x.start()
    other_x = pltpu.make_async_remote_copy(
        src_ref=x_own, dst_ref=x_all.at[pl.ds(tok, tok)], send_sem=x_sem.at[1], recv_sem=x_sem.at[2],
        device_id=(1 - me_c, me_f), device_id_type=MESH)
    other_x.start()

    def all_sends(waiting):
        def send(src, k, c, p, sem):
            move(src, land.at[CSLOT[k] + p % (TPD[k])], sem, recv_tile.at[k], c, p // (TPD[k]), waiting)

        @pl.when(dev < FIRST_W2)
        def _():
            first = row_start(dev)

            def per_row(t, carry):
                row = first + t
                for k in range(len(CHUNKS)):
                    n = CHUNKS[k]

                    def per_col(j, carry2):
                        for c in range(2):
                            p = ((row // 2) * n + j) * 2 + row % 2
                            send(src13.at[eight(t), HB * c + OFFS[k] + j, 0], k, c, p, send13.at[t])
                        return carry2

                    repeat(n, per_col)
                return carry

            repeat(row_start(dev + 1) - first, per_row)

        @pl.when(dev >= FIRST_W2)
        def _():
            first = w2_row_start(dev)

            def per_row(t, carry):
                row = first + t
                c = row // FT
                kk = row % FT
                for k in range(len(CHUNKS)):
                    n = CHUNKS[k]

                    @pl.when((kk >= 16 * OFFS[k]) & (kk < 16 * (OFFS[k] + n)))
                    def _():
                        local = kk - 16 * OFFS[k]

                        def per_col(j, carry2):
                            p = 2 * DT * n + ((local // 2) * ND + j) * 2 + local % 2
                            send(src2.at[eight(t), j, 0], k, c, p, send2.at[t])
                            return carry2

                        repeat(ND, per_col)
                return carry

            repeat(w2_row_start(dev + 1) - first, per_row)

        @pl.when(dev == 0)
        def _():
            def per_device(d, carry):
                move(gain_src.at[0, head(8), 0], gain_land, send_gain, recv_gain, d // GRP, d % GRP, waiting)
                return carry

            repeat(NDEV, per_device)

    all_sends(False)

    for k in range(len(CHUNKS)):
        tiles = 3 * DT * CHUNKS[k]
        whole, rest = tiles // (TPD[k]), tiles % (TPD[k])

        @pl.when(me_f < whole)
        def _():
            part = land.at[pl.ds(CSLOT[k], TPD[k])]
            pltpu.make_async_copy(part, part, recv_tile.at[k]).wait()

        if rest:
            @pl.when(me_f == whole)
            def _():
                part = land.at[pl.ds(CSLOT[k], rest)]
                pltpu.make_async_copy(part, part, recv_tile.at[k]).wait()
        for colour in COLOURS:
            first, inside, count = unit_range(k, colour)
            value = land[CSLOT[k] + 2 * inside:CSLOT[k] + 2 * (inside + count)]
            mine[first:first + count] = value.reshape(count, *UNIT).astype(jnp.bfloat16)
    local = pltpu.make_async_copy(mine, out.at[pos['z'], pos['y'], pos['x']], local_sem)
    local.start()
    local.wait()

    def axis_of(colour, phase):
        return AXES[(2 - colour - phase) % 3]

    def ring_copies(colour, phase, step, first, count, sem):
        axis = axis_of(colour, phase)
        done = [axis_of(colour, q) for q in range(phase)]
        made = []
        for way, shift in enumerate(WAYS):
            where = {a: pos[a] for a in AXES if a not in done}
            low, size = first, count
            if step == 1:
                where[axis] = (pos[axis] - shift + 4) % 4
                size = (count + 1) // 2 if way == 0 else count // 2
                low = first if way == 0 else first + (count + 1) // 2
            index = block_set(where, low, size)
            made.append(pltpu.make_async_remote_copy(
                src_ref=out.at[index],
                dst_ref=out.at[index],
                send_sem=send_sem.at[sem, step, way],
                recv_sem=recv_sem.at[sem, step, way],
                device_id=neighbour(pos, axis, shift),
                device_id_type=MESH,
            ))
        return made

    def start_all(copies):
        for copy in copies:
            copy.start()

    def wait_all(copies):
        for copy in copies:
            copy.wait()

    def early(phase, step):
        return [c for j in COLOURS for c in ring_copies(j, phase, step, COL_BASE[j], COL_LEN[j], phase * 3 + j)]

    def late(k, step):
        made = []
        for j in COLOURS:
            first, _, count = unit_range(k, j)
            made += ring_copies(j, 2, step, first, count, 6 + k * 3 + j)
        return made

    start_all(early(0, 0))
    pltpu.make_async_copy(gain_land, gain_land, recv_gain).wait()
    own_x.wait()
    other_x.wait()
    gain = jnp.concatenate([gain_land[i:i + 1, :] for i in range(ND)], axis=1).astype(jnp.bfloat16).astype(jnp.float32)

    def normalise(t, carry):
        rows = pl.ds(pl.multiple_of(t * 256, 256), 256)
        hidden = x_all[rows, :].astype(jnp.float32)
        inv_rms = lax.rsqrt(jnp.mean(hidden * hidden, axis=-1, keepdims=True) + RMS_EPS)
        normed = hidden * inv_rms * gain
        u_all[rows, :] = normed.astype(jnp.bfloat16)
        u_t[:, rows] = normed.T.astype(jnp.bfloat16)
        return carry

    half_tiles = x_all.shape[0] // 512
    repeat(half_tiles, normalise)
    wait_all(early(0, 0))
    start_all(early(0, 1))
    lax.fori_loop(half_tiles, 2 * half_tiles, normalise, 0)
    wait_all(early(0, 1))
    start_all(early(1, 0))
    u_save = pltpu.make_async_copy(u_all, u_out, save_sem.at[0])
    x_save = pltpu.make_async_copy(x_all, x_out, save_sem.at[1])
    t_save = pltpu.make_async_copy(u_t, t_out, save_sem.at[3])
    u_save.start()
    x_save.start()
    t_save.start()
    wait_all(early(1, 0))
    start_all(early(1, 1))
    wait_all(early(1, 1))

    def loads(k):
        made = []
        for j in COLOURS:
            first, inside, count = unit_range(k, j)
            made.append(pltpu.make_async_copy(
                out.at[:, :, :, pl.ds(first, count)], wbuf.at[k % 2, :, :, :, pl.ds(inside, count)], load_sem.at[k % 2, j]))
        return made

    def compute(k):
        n = CHUNKS[k]

        def tile(t, carry):
            rows = pl.ds(pl.multiple_of(t * TOK_TILE, TOK_TILE), TOK_TILE)
            w_one, w_three, w_two = chunk_matrices(wbuf[k % 2, :, :, :, 0:CU[k]], n)
            u = u_all[rows, :]
            gate = jnp.dot(u, w_one, preferred_element_type=jnp.float32)
            up = jnp.dot(u, w_three, preferred_element_type=jnp.float32)
            inner = (gate * jax.nn.sigmoid(gate) * up).astype(jnp.bfloat16)
            piece = jnp.dot(inner, w_two, preferred_element_type=jnp.float32)
            h_acc[rows, :] = piece if k == 0 else h_acc[rows, :] + piece
            return carry

        repeat(x_all.shape[0] // TOK_TILE, tile)

    last = len(CHUNKS) - 1
    start_all(late(0, 0))
    start_all(late(1, 0))
    for k in range(last + 1):
        wait_all(late(k, 0))
        start_all(late(k, 1))
        if k + 2 <= last:
            start_all(late(k + 2, 0))
        if k >= 1:
            wait_all(loads(k - 1))
            compute(k - 1)
        wait_all(late(k, 1))
        start_all(loads(k))
    wait_all(loads(last))
    compute(last)
    h_saves = [pltpu.make_async_copy(h_acc.at[pl.ds(tok * i, tok)], dst, h_sem.at[i]) for i, dst in enumerate((h_mine, h_other))]
    start_all(h_saves)
    wait_all(h_saves)
    u_save.wait()
    x_save.wait()
    t_save.wait()
    all_sends(True)


def forward_tiles(al13, al2, gain_tile, x_own):
    tok = 2 * x_own.shape[0]
    return pl.pallas_call(
        forward_kernel,
        out_shape=(
            jax.ShapeDtypeStruct((4, 4, 4, UNITS, *UNIT), jnp.bfloat16),
            jax.ShapeDtypeStruct(x_own.shape, jnp.float32),
            jax.ShapeDtypeStruct(x_own.shape, jnp.float32),
            jax.ShapeDtypeStruct((tok, D), jnp.bfloat16),
            jax.ShapeDtypeStruct((D, tok), jnp.bfloat16),
            jax.ShapeDtypeStruct((tok, D), jnp.bfloat16),
        ),
        in_specs=[pl.BlockSpec(memory_space=pltpu.VMEM)] * 3 + [pl.BlockSpec(memory_space=pl.ANY)],
        out_specs=[pl.BlockSpec(memory_space=pl.ANY)] * 6,
        scratch_shapes=[
            pltpu.VMEM((CSLOTS, *TILE), jnp.float32),
            pltpu.VMEM((UNITS, *UNIT), jnp.bfloat16),
            pltpu.VMEM(TILE, jnp.float32),
            pltpu.VMEM((tok, D), jnp.bfloat16),
            pltpu.VMEM((tok, D), jnp.bfloat16),
            pltpu.VMEM((D, tok), jnp.bfloat16),
            pltpu.VMEM((tok, D), jnp.float32),
            pltpu.VMEM((2, 4, 4, 4, max(CU), *UNIT), jnp.bfloat16),
            pltpu.SemaphoreType.DMA((3,)),
            pltpu.SemaphoreType.DMA((15,)),
            pltpu.SemaphoreType.DMA,
            pltpu.SemaphoreType.DMA((len(CHUNKS),)),
            pltpu.SemaphoreType.DMA,
            pltpu.SemaphoreType.DMA((3,)),
            pltpu.SemaphoreType.DMA,
            pltpu.SemaphoreType.DMA((2, 3)),
            pltpu.SemaphoreType.DMA((4,)),
            pltpu.SemaphoreType.DMA((2,)),
            pltpu.SemaphoreType.DMA((6 + 3 * len(CHUNKS), 2, 2)),
            pltpu.SemaphoreType.DMA((6 + 3 * len(CHUNKS), 2, 2)),
        ],
        compiler_params=pltpu.CompilerParams(has_side_effects=True, vmem_limit_bytes=60 * 2 ** 20),
        name='forward_tiles',
    )(al13, al2, gain_tile, x_own)


def cut_tiles(count):
    sizes = [(count + 2 - j) // 3 for j in COLOURS]
    return tuple((sum(sizes[:j]), sizes[j]) for j in COLOURS)


def nt(a, b):
    return lax.dot_general(a, b, (((1,), (1,)), ((), ())), preferred_element_type=jnp.float32)


def backward_kernel(units, u_hbm, t_hbm, x_hbm, e_mine, e_other, loss_tile, out13, out2, out_gain,
                    total, relay0, relay1, relay2, merge0, merge1, merge2, ring_sum, final, wbuf, u_all, u_t, x_all, e_all, r_all,
                    d_gate, d_up, inner, gain_acc,
                    load_sem, w_sem, send_sem, recv_sem, send_tile, send_gain, recv13, recv2, recv_gain, credit):
    dev = my_index()
    me_c = lax.axis_index('dp')
    me_f = lax.axis_index('fsdp')
    pos = ring_pos()
    relays = (relay0, relay1, relay2)
    merges = (merge0, merge1, merge2)
    tok = u_all.shape[0]

    def weight_loads(i):
        k = ORDER[i]
        made = []
        for j in COLOURS:
            first, inside, count = unit_range(k, j)
            made.append(pltpu.make_async_copy(
                units.at[:, :, :, pl.ds(first, count)], wbuf.at[i % 2, :, :, :, pl.ds(inside, count)], w_sem.at[i % 2, j]))
        return made

    def start_all(copies):
        for copy in copies:
            copy.start()

    def wait_all(copies):
        for copy in copies:
            copy.wait()

    inputs = [pltpu.make_async_copy(src, dst, load_sem.at[i])
              for i, (src, dst) in enumerate((
                  (u_hbm, u_all), (e_mine, e_all.at[head(tok // 2)]), (e_other, e_all.at[pl.ds(tok // 2, tok // 2)]),
                  (x_hbm, x_all), (t_hbm, u_t)))]
    start_all(weight_loads(0))
    start_all(inputs)

    def axis_of(colour, phase):
        return AXES[(colour + phase) % 3]

    def set_ref(i, colour, phase, at, rows):
        first = axis_of(colour, 0)
        tiles = (pl.ds(*rows),)
        if phase == 0:
            return total.at[(i % 2,) + tuple(at if a == first else slice(None) for a in AXES) + tiles]
        fixed = {axis_of(colour, q): pos[axis_of(colour, q)] for q in range(phase)}
        fixed[axis_of(colour, phase)] = at
        spot = tuple(fixed.get(a, slice(None)) for a in AXES if a != first)
        return ring_sum.at[(i % 3, colour) + spot + (pl.ds(rows[0] - cut_tiles(TPD[ORDER[i]])[colour][0], rows[1]),)]

    def rows_of(i, colour, way):
        first, size = cut_tiles(TPD[ORDER[i]])[colour]
        half = (size + 1) // 2
        return ((first, half), (first + half, size - half), (first, size))[way]

    def copies(i, colour, phase, step):
        axis = axis_of(colour, phase)
        made = []
        for way, shift in enumerate(WAYS):
            rows = rows_of(i, colour, way if step == 0 else 2)
            at = (pos[axis] + (2 if step == 0 else shift + 4)) % 4
            dst = (relays if step == 0 else merges)[phase]
            lead = (i % 2, colour, way) + (slice(None),) * (2 - phase)
            sem = (i % 2, colour * 3 + phase, step, way)
            made.append(pltpu.make_async_remote_copy(
                src_ref=set_ref(i, colour, phase, at, rows),
                dst_ref=dst.at[lead + (head(rows[1]),)],
                send_sem=send_sem.at[sem],
                recv_sem=recv_sem.at[sem],
                device_id=neighbour(pos, axis, shift),
                device_id_type=MESH,
            ))
        return made

    def add_set(i, colour, phase, at, rows, landed, done):
        src = set_ref(i, colour, phase, at, rows)

        def body(b, carry):
            spot = ((b // 4, b % 4), (b,), ())[phase]
            value = src[spot + (slice(None),)]
            for part in landed:
                value = value + part[spot + (head(rows[1]),)]
            if not done or phase == 1:
                src[spot + (slice(None),)] = value
            elif phase == 0:
                ring_sum[(i % 3, colour) + spot + (head(rows[1]),)] = value
            else:
                final[i, pl.ds(*rows)] = value
            return carry

        repeat(4 ** (2 - phase), body)

    def tell_neighbours(sem):
        for axis in AXES:
            for shift in WAYS:
                pl.semaphore_signal(sem, inc=1, device_id=neighbour(pos, axis, shift), device_id_type=MESH)

    def reduce_step(i, s):
        if s < 3 and i >= 2:
            pl.semaphore_wait(credit.at[s, i - 2], 6)
        for colour in COLOURS:
            if s > 0:
                phase, step = (s - 1) // 2, (s - 1) % 2
                here = pos[axis_of(colour, phase)]
                wait_all(copies(i, colour, phase, step))
                if step == 0:
                    for way, shift in enumerate((1, 3)):
                        add_set(i, colour, phase, (here + shift) % 4, rows_of(i, colour, way), [relays[phase].at[i % 2, colour, way]], False)
                else:
                    add_set(i, colour, phase, here, rows_of(i, colour, 2),
                            [merges[phase].at[i % 2, colour, way] for way in range(2)], True)
            if s < 6:
                start_all(copies(i, colour, s // 2, s % 2))
        if i + 2 < len(ORDER) and s in (1, 2, 6):
            tell_neighbours(credit.at[min(s, 3) - 1, i])
        if s == 6:
            send_home(i, False)

    def send_home(i, waiting):
        k = ORDER[i]
        n = CHUNKS[k]
        own = TPD[k]

        def per_slot(slot, carry):
            p = me_f * own + slot

            @pl.when(p < 2 * DT * n)
            def _():
                q = p // 2
                row = (q // n) * 2 + p % 2
                owner = (8 * row) // 21
                t = row - row_start(owner)
                dst = out13.at[eight(t), HB * me_c + OFFS[k] + q % n, 0]
                move(final.at[i, slot], dst, send_tile.at[i], recv13.at[t], owner // GRP, owner % GRP, waiting)

            @pl.when(p >= 2 * DT * n)
            def _():
                q = (p - 2 * DT * n) // 2
                row = FT * me_c + 16 * OFFS[k] + (q // ND) * 2 + p % 2
                owner = FIRST_W2 + (8 * row + 38) // 114
                t = row - w2_row_start(owner)
                dst = out2.at[eight(t), q % ND, 0]
                move(final.at[i, slot], dst, send_tile.at[i], recv2.at[t], owner // GRP, owner % GRP, waiting)
            return carry

        repeat(jnp.clip(3 * DT * n - me_f * own, 0, own), per_slot)
        if k == 0:
            @pl.when(me_f == GAIN_F)
            def _():
                def per_device(d, carry):
                    move(final.at[i, 0], out_gain.at[me_c], send_gain, recv_gain.at[me_c], d // GRP, d % GRP, waiting)
                    return carry

                repeat(NDEV, per_device)

    def store_tiles(i, first, value):
        own = CU[ORDER[i]]
        count = value.shape[0]
        for f in range(first // own, (first + count + own - 1) // own):
            low, high = max(first, f * own), min(first + count, (f + 1) * own)
            part = value[low - first:high - first].reshape((high - low) * 2, *TILE)
            z, y, x = coords(f)
            total[i % 2, z, y, x, pl.ds((low - f * own) * 2, (high - low) * 2)] = part

    def to_units(matrix):
        blocks = matrix.shape[1] // 128
        cols = [matrix[:, lanes(j)].reshape(-1, 1, *UNIT) for j in range(blocks)]
        return jnp.concatenate(cols, axis=1).reshape(-1, *UNIT)

    def token_tile(i, t, hooks):
        n = CHUNKS[ORDER[i]]
        width = LANES * n
        rows = pl.ds(pl.multiple_of(t * TOK_TILE, TOK_TILE), TOK_TILE)
        w_one, w_three, w_two = chunk_matrices(wbuf[i % 2, :, :, :, 0:CU[ORDER[i]]], n)
        u = u_all[rows, :]
        gate = jnp.dot(u, w_one, preferred_element_type=jnp.float32)
        up = jnp.dot(u, w_three, preferred_element_type=jnp.float32)
        d_inner = nt(e_all[rows, :], w_two)
        sig = jax.nn.sigmoid(gate)
        silu = gate * sig
        inner[rows, 0:width] = (silu * up).astype(jnp.bfloat16)
        dg = (d_inner * up * sig * (1.0 + gate * (1.0 - sig))).astype(jnp.bfloat16)
        du = (d_inner * silu).astype(jnp.bfloat16)
        d_gate[rows, 0:width] = dg
        d_up[rows, 0:width] = du
        q = nt(dg, w_one) + nt(du, w_three)
        x = x_all[rows, :].astype(jnp.float32)
        if i == 0:
            r_all[rows, :] = lax.rsqrt(jnp.mean(x * x, axis=-1, keepdims=True) + RMS_EPS)
        piece = (q * (x * r_all[rows, :])).reshape(TOK_TILE // 8, 8, D)
        gain_acc[...] += jnp.sum(piece, axis=0)
        for at, hook in hooks:
            pl.when(t == at)(hook)

    gain_acc[...] = jnp.zeros_like(gain_acc)
    wait_all(inputs)
    for i in range(len(ORDER)):
        k = ORDER[i]
        n = CHUNKS[k]
        width = LANES * n
        wait_all(weight_loads(i))
        if i + 1 < len(ORDER):
            start_all(weight_loads(i + 1))
        plan = [tuple(map(int, HOOKS[at:at + 3])) for at in range(0, len(HOOKS), 3)]
        hooks = [(at, functools.partial(reduce_step, i - back, s)) for at, back, s in plan if i >= back]

        def tile(t, carry, i=i, hooks=hooks):
            token_tile(i, t, hooks)
            return carry

        repeat(tok // TOK_TILE, tile)
        store_tiles(i, 0, to_units(jnp.dot(u_t[...], d_gate[:, 0:width], preferred_element_type=jnp.float32)))
        store_tiles(i, DU * n, to_units(jnp.dot(u_t[...], d_up[:, 0:width], preferred_element_type=jnp.float32)))
        d_two = lax.dot_general(inner[:, 0:width], e_all[...], (((0,), (0,)), ((), ())), preferred_element_type=jnp.float32)
        store_tiles(i, 2 * DU * n, to_units(d_two))
        if k == 0:
            d_gain = jnp.sum(gain_acc[...], axis=0, keepdims=True)
            rows = [d_gain[:, lanes(j)] for j in range(ND)]
            total[i % 2, 3, 3, 3, 0] = jnp.concatenate(rows + [loss_tile[7:8, :]], axis=0)
        reduce_step(i, 0)

    last = len(ORDER) - 1
    for back, s in zip(DRAIN[::2], DRAIN[1::2]):
        reduce_step(last - int(back), int(s))
    for i in range(len(ORDER)):
        send_home(i, True)

    @pl.when(dev < FIRST_W2)
    def _():
        def wait_row(t, carry):
            part = out13.at[eight(t)]
            pltpu.make_async_copy(part, part, recv13.at[t]).wait()
            return carry

        repeat(row_start(dev + 1) - row_start(dev), wait_row)

    @pl.when(dev >= FIRST_W2)
    def _():
        def wait_row(t, carry):
            part = out2.at[eight(t)]
            pltpu.make_async_copy(part, part, recv2.at[t]).wait()
            return carry

        repeat(w2_row_start(dev + 1) - w2_row_start(dev), wait_row)

    for c in range(2):
        pltpu.make_async_copy(out_gain.at[c], out_gain.at[c], recv_gain.at[c]).wait()


def backward_tiles(units, u, u_t, x, err, err_other, loss_tile):
    tok = u.shape[0]
    width = 128 * max(CHUNKS)
    relays = [pltpu.VMEM((2, 3, 2) + (4,) * (2 - p) + (HALF, *TILE), jnp.float32) for p in COLOURS]
    merges = [pltpu.VMEM((2, 3, 2) + (4,) * (2 - p) + (FULL, *TILE), jnp.float32) for p in COLOURS]
    bf16_act = pltpu.VMEM((tok, D), jnp.bfloat16)
    chunk_act = pltpu.VMEM((tok, width), jnp.bfloat16)
    dma = pltpu.SemaphoreType.DMA
    return pl.pallas_call(
        backward_kernel,
        out_shape=(
            jax.ShapeDtypeStruct((ROWS13, NB, 1, LANES), jnp.float32),
            jax.ShapeDtypeStruct((ROWS2, ND, 1, LANES), jnp.float32),
            jax.ShapeDtypeStruct((2, *TILE), jnp.float32),
        ),
        in_specs=[pl.BlockSpec(memory_space=pl.ANY)] * 6 + [pl.BlockSpec(memory_space=pltpu.VMEM)],
        out_specs=[pl.BlockSpec(memory_space=pl.ANY)] * 3,
        scratch_shapes=[
            pltpu.VMEM((2, 4, 4, 4, max(TPD), *TILE), jnp.float32),
            *relays,
            *merges,
            pltpu.VMEM((3, 3, 4, 4, FULL, *TILE), jnp.float32),
            pltpu.VMEM((len(ORDER), max(TPD), *TILE), jnp.float32),
            pltpu.VMEM((2, 4, 4, 4, max(CU), *UNIT), jnp.bfloat16),
            bf16_act,
            pltpu.VMEM((D, tok), jnp.bfloat16),
            bf16_act,
            bf16_act,
            pltpu.VMEM((tok, 1), jnp.float32),
            chunk_act,
            chunk_act,
            chunk_act,
            pltpu.VMEM((8, D), jnp.float32),
            dma((5,)),
            dma((2, 3)),
            dma((2, 9, 2, 2)),
            dma((2, 9, 2, 2)),
            dma((len(ORDER),)),
            dma,
            dma((3,)),
            dma((15,)),
            dma((2,)),
            pltpu.SemaphoreType.REGULAR((3, len(ORDER))),
        ],
        compiler_params=pltpu.CompilerParams(has_side_effects=True, vmem_limit_bytes=63 * 2 ** 20),
        name='backward_tiles',
    )(units, u, u_t, x, err, err_other, loss_tile)


def region_offset(dev):
    first13 = D + 8 * FF * row_start(dev)
    first2 = W2_START + 8 * D * w2_row_start(dev)
    return jnp.where(dev <= FIRST_W2, first13, first2) - SHARD * dev


def adam_update(master, adam_m, adam_v, grad_mean):
    m_new = BETA_ONE * adam_m + (1.0 - BETA_ONE) * grad_mean
    v_new = BETA_TWO * adam_v + (1.0 - BETA_TWO) * grad_mean * grad_mean
    m_hat = m_new / (1.0 - BETA_ONE ** ADAM_STEP)
    v_hat = v_new / (1.0 - BETA_TWO ** ADAM_STEP)
    master_new = master - LEARN_RATE * (m_hat / (jnp.sqrt(v_hat) + ADAM_EPS) + DECAY_RATE * master)
    return master_new, m_new, v_new


def aligned_region(own):
    dev = my_index()
    ring = [(i, (i - 1) % NDEV) for i in range(NDEV)]
    spill = lax.ppermute(own[:SPILL], ('dp', 'fsdp'), ring)
    start = region_offset(dev)
    longer = jnp.concatenate([own, spill, jnp.zeros((SPILL + AL_LEN - SHARD - SPILL,), jnp.float32)])
    aligned = lax.dynamic_slice(longer, (start,), (AL_LEN,))
    al13 = aligned.reshape(ROWS13, NB, 1, LANES)
    al2 = aligned[:ROWS2 * D].reshape(ROWS2, ND, 1, LANES)
    gain_tile = own[:1024].reshape(1, 8, 1, LANES)
    return al13, al2, gain_tile


def solution(mesh):
    flat_spec = P(None, ('dp', 'fsdp'))
    act_spec = P(None, ('dp', 'fsdp'), None, None)
    swap = [(0, 1), (1, 0)]

    def train_step(master, adam_m, adam_v, inputs, targets):
        token_total = inputs.shape[1] * inputs.shape[2]

        def local_step(master_sh, m_sh, v_sh, x_loc, y_loc):
            dev = my_index()
            tok = x_loc.shape[1] * x_loc.shape[2]
            own = master_sh.reshape(SHARD)
            x_own = x_loc.reshape(tok, D)
            y_own = y_loc.reshape(tok, D)
            al13, al2, gain_tile = aligned_region(own)
            units, h_mine, h_other, normed, normed_t, x_all = forward_tiles(al13, al2, gain_tile, x_own)
            other = lax.ppermute(h_other, 'dp', swap)
            err = x_own.astype(jnp.float32) + (h_mine + other) - y_own.astype(jnp.float32)
            loss_sum = 0.5 * jnp.sum(err * err)
            err_b = err.astype(jnp.bfloat16)
            err_other = lax.ppermute(err_b, 'dp', swap)

            loss_tile = jnp.pad(loss_sum.reshape(1), (D, 127)).reshape(TILE)
            out13, out2, out_gain = backward_tiles(units, normed, normed_t, x_all, err_b, err_other, loss_tile)
            sums = (out_gain[0] + out_gain[1]).reshape(1024)
            loss_value = sums[D] / token_total
            flat13 = out13.reshape(AL_LEN)
            flat2 = jnp.pad(out2.reshape(ROWS2 * D), (0, AL_LEN - ROWS2 * D))
            aligned = jnp.where(dev < FIRST_W2, flat13, flat2)
            start = region_offset(dev)
            longer = jnp.concatenate([jnp.zeros((SPILL,), jnp.float32), aligned, jnp.zeros((SPILL,), jnp.float32)])
            spill = lax.dynamic_slice(longer, (SPILL + SHARD - start,), (SPILL,))
            body = lax.dynamic_slice(longer, (SPILL - start,), (SHARD,))
            ring = [(i, (i + 1) % NDEV) for i in range(NDEV)]
            head = lax.ppermute(spill, ('dp', 'fsdp'), ring)
            head = jnp.where(dev == 0, jnp.pad(sums[:D], (0, SPILL - D)), head)
            grad_sum = jnp.where(jnp.arange(SHARD) < start, jnp.pad(head, (0, SHARD - SPILL)), body)
            grad_mean = grad_sum.reshape(1, SHARD) / token_total
            master_new, m_new, v_new = adam_update(master_sh, m_sh, v_sh, grad_mean)
            return master_new, m_new, v_new, loss_value

        return jax.shard_map(local_step, mesh=mesh, in_specs=(flat_spec, flat_spec, flat_spec, act_spec, act_spec), out_specs=(flat_spec, flat_spec, flat_spec, P()), check_vma=False)(master, adam_m, adam_v, inputs, targets)

    return train_step
```

```python
import functools

import jax
import jax.numpy as jnp
from jax import lax
from jax.experimental import pallas as pl
from jax.experimental.pallas import tpu as pltpu
from jax.sharding import PartitionSpec as P

ADAM_STEP = 3
LEARN_RATE = 2e-3
BETA_ONE = 0.9
BETA_TWO = 0.999
ADAM_EPS = 1e-8
DECAY_RATE = 0.1
RMS_EPS = 1e-5

D = 896
FF = 4864
FLAT = D * (3 * FF + 1)
NDEV = 128
GRP = 64
SHARD = FLAT // NDEV
NB = FF // 128
ND = D // 128
LANES = 128
TILE = (8, LANES)
UNIT = (16, LANES)
DT = D // 8
DU = D // 16
FT = FF // 16
HB = NB // 2
W2_START = D + 2 * D * FF
FIRST_W2 = 85
SPILL = 35840
ROWS13, ROWS2 = 24, 120
AL_LEN = ROWS13 * FF

CHUNKS = (3, 4, 4, 4, 4)
OFFS = tuple(sum(CHUNKS[:k]) for k in range(len(CHUNKS)))
CU = (8, 11, 11, 11, 11)
TPD = tuple(2 * u for u in CU)
CSLOT = tuple(sum(TPD[:k]) for k in range(len(CHUNKS)))
CSLOTS = sum(TPD)
UNITS = sum(CU)
COLOURS = range(3)
CCOL = tuple(tuple(int('332443344434443'[3 * k + j]) for j in COLOURS) for k in range(len(CHUNKS)))
COL_LEN = tuple(sum(c[j] for c in CCOL) for j in COLOURS)
COL_BASE = (0, COL_LEN[0], COL_LEN[0] + COL_LEN[1])
TOK_TILE = 512

ORDER = (1, 2, 3, 4, 0)
WAYS = (1, -1)
HOOKS = '046122234211323335'
DRAIN = '361224011325261402150316040506'
GAIN_F = GRP - 1
HALF, FULL = 4, 8
AXES = ('z', 'y', 'x')

MESH = pl.DeviceIdType.MESH


def row_start(dev):
    return (21 * dev + 7) // 8


def w2_row_start(dev):
    return jnp.maximum((114 * dev - 9728 + 7) // 8, 0)


def repeat(count, body):
    lax.fori_loop(0, count, body, 0)


def lanes(j):
    return slice(j * LANES, (j + 1) * LANES)


def head(count):
    return pl.ds(0, count)


def eight(t):
    return pl.ds(t * 8, 8)


def my_index():
    return lax.axis_index('dp') * GRP + lax.axis_index('fsdp')


def move(src, dst, send_sem, recv_sem, c, f, waiting):
    stays = (c == lax.axis_index('dp')) & (f == lax.axis_index('fsdp'))

    def remote():
        return pltpu.make_async_remote_copy(
            src_ref=src, dst_ref=dst, send_sem=send_sem, recv_sem=recv_sem, device_id=(c, f), device_id_type=MESH)

    if waiting:
        @pl.when(jnp.logical_not(stays))
        def _():
            remote().wait_send()
    else:
        @pl.when(jnp.logical_not(stays))
        def _():
            remote().start()

        @pl.when(stays)
        def _():
            pltpu.make_async_copy(src, dst, recv_sem).start()


def coords(f):
    return f // 16, (f // 4) % 4, f % 4


def ring_pos():
    f = lax.axis_index('fsdp')
    return dict(zip(AXES, coords(f)))


def neighbour(pos, axis, step):
    moved = dict(pos)
    moved[axis] = (pos[axis] + step + 4) % 4
    return (lax.axis_index('dp'), moved['z'] * 16 + moved['y'] * 4 + moved['x'])


def unit_range(k, colour):
    first = COL_BASE[colour] + sum(c[colour] for c in CCOL[:k])
    inside = sum(CCOL[k][:colour])
    return first, inside, CCOL[k][colour]


def block_set(fixed, first, count):
    return tuple(fixed.get(axis, slice(None)) for axis in AXES) + (pl.ds(first, count),)


def chunk_matrices(units, n):
    flat = units.reshape(-1, *UNIT)
    part = DU * n

    def matrix(low, rows, blocks):
        tiles = flat[low:low + rows * blocks].reshape(rows, blocks, *UNIT)
        return jnp.concatenate([tiles[:, j].reshape(rows * 16, 128) for j in range(blocks)], axis=1)

    return matrix(0, DU, n), matrix(part, DU, n), matrix(2 * part, 8 * n, ND)


def forward_kernel(src13, src2, gain_src, x_own, out, h_mine, h_other, u_out, t_out, x_out, land, mine, gain_land, x_all, u_all, u_t, h_acc, wbuf,
                   send13, send2, send_gain, recv_tile, recv_gain, x_sem, local_sem, load_sem, save_sem, h_sem, send_sem, recv_sem):
    dev = my_index()
    me_c = lax.axis_index('dp')
    me_f = lax.axis_index('fsdp')
    pos = ring_pos()
    tok = x_own.shape[0]

    own_x = pltpu.make_async_copy(x_own, x_all.at[pl.ds(0, tok)], x_sem.at[0])
    own_x.start()
    other_x = pltpu.make_async_remote_copy(
        src_ref=x_own, dst_ref=x_all.at[pl.ds(tok, tok)], send_sem=x_sem.at[1], recv_sem=x_sem.at[2],
        device_id=(1 - me_c, me_f), device_id_type=MESH)
    other_x.start()

    def all_sends(waiting):
        def send(src, k, c, p, sem):
            move(src, land.at[CSLOT[k] + p % (TPD[k])], sem, recv_tile.at[k], c, p // (TPD[k]), waiting)

        @pl.when(dev < FIRST_W2)
        def _():
            first = row_start(dev)

            def per_row(t, carry):
                row = first + t
                for k in range(len(CHUNKS)):
                    n = CHUNKS[k]

                    def per_col(j, carry2):
                        for c in range(2):
                            p = ((row // 2) * n + j) * 2 + row % 2
                            send(src13.at[eight(t), HB * c + OFFS[k] + j, 0], k, c, p, send13.at[t])
                        return carry2

                    repeat(n, per_col)
                return carry

            repeat(row_start(dev + 1) - first, per_row)

        @pl.when(dev >= FIRST_W2)
        def _():
            first = w2_row_start(dev)

            def per_row(t, carry):
                row = first + t
                c = row // FT
                kk = row % FT
                for k in range(len(CHUNKS)):
                    n = CHUNKS[k]

                    @pl.when((kk >= 16 * OFFS[k]) & (kk < 16 * (OFFS[k] + n)))
                    def _():
                        local = kk - 16 * OFFS[k]

                        def per_col(j, carry2):
                            p = 2 * DT * n + ((local // 2) * ND + j) * 2 + local % 2
                            send(src2.at[eight(t), j, 0], k, c, p, send2.at[t])
                            return carry2

                        repeat(ND, per_col)
                return carry

            repeat(w2_row_start(dev + 1) - first, per_row)

        @pl.when(dev == 0)
        def _():
            def per_device(d, carry):
                move(gain_src.at[0, head(8), 0], gain_land, send_gain, recv_gain, d // GRP, d % GRP, waiting)
                return carry

            repeat(NDEV, per_device)

    all_sends(False)

    for k in range(len(CHUNKS)):
        tiles = 3 * DT * CHUNKS[k]
        whole, rest = tiles // (TPD[k]), tiles % (TPD[k])

        @pl.when(me_f < whole)
        def _():
            part = land.at[pl.ds(CSLOT[k], TPD[k])]
            pltpu.make_async_copy(part, part, recv_tile.at[k]).wait()

        if rest:
            @pl.when(me_f == whole)
            def _():
                part = land.at[pl.ds(CSLOT[k], rest)]
                pltpu.make_async_copy(part, part, recv_tile.at[k]).wait()
        for colour in COLOURS:
            first, inside, count = unit_range(k, colour)
            value = land[CSLOT[k] + 2 * inside:CSLOT[k] + 2 * (inside + count)]
            mine[first:first + count] = value.reshape(count, *UNIT).astype(jnp.bfloat16)
    local = pltpu.make_async_copy(mine, out.at[pos['z'], pos['y'], pos['x']], local_sem)
    local.start()
    local.wait()

    def axis_of(colour, phase):
        return AXES[(2 - colour - phase) % 3]

    def ring_copies(colour, phase, step, first, count, sem):
        axis = axis_of(colour, phase)
        done = [axis_of(colour, q) for q in range(phase)]
        made = []
        for way, shift in enumerate(WAYS):
            where = {a: pos[a] for a in AXES if a not in done}
            low, size = first, count
            if step == 1:
                where[axis] = (pos[axis] - shift + 4) % 4
                size = (count + 1) // 2 if way == 0 else count // 2
                low = first if way == 0 else first + (count + 1) // 2
            index = block_set(where, low, size)
            made.append(pltpu.make_async_remote_copy(
                src_ref=out.at[index],
                dst_ref=out.at[index],
                send_sem=send_sem.at[sem, step, way],
                recv_sem=recv_sem.at[sem, step, way],
                device_id=neighbour(pos, axis, shift),
                device_id_type=MESH,
            ))
        return made

    def start_all(copies):
        for copy in copies:
            copy.start()

    def wait_all(copies):
        for copy in copies:
            copy.wait()

    def early(phase, step):
        return [c for j in COLOURS for c in ring_copies(j, phase, step, COL_BASE[j], COL_LEN[j], phase * 3 + j)]

    def late(k, step):
        made = []
        for j in COLOURS:
            first, _, count = unit_range(k, j)
            made += ring_copies(j, 2, step, first, count, 6 + k * 3 + j)
        return made

    start_all(early(0, 0))
    pltpu.make_async_copy(gain_land, gain_land, recv_gain).wait()
    own_x.wait()
    other_x.wait()
    gain = jnp.concatenate([gain_land[i:i + 1, :] for i in range(ND)], axis=1).astype(jnp.bfloat16).astype(jnp.float32)

    def normalise(t, carry):
        rows = pl.ds(pl.multiple_of(t * 256, 256), 256)
        hidden = x_all[rows, :].astype(jnp.float32)
        inv_rms = lax.rsqrt(jnp.mean(hidden * hidden, axis=-1, keepdims=True) + RMS_EPS)
        normed = hidden * inv_rms * gain
        u_all[rows, :] = normed.astype(jnp.bfloat16)
        u_t[:, rows] = normed.T.astype(jnp.bfloat16)
        return carry

    half_tiles = x_all.shape[0] // 512
    repeat(half_tiles, normalise)
    wait_all(early(0, 0))
    start_all(early(0, 1))
    lax.fori_loop(half_tiles, 2 * half_tiles, normalise, 0)
    wait_all(early(0, 1))
    start_all(early(1, 0))
    u_save = pltpu.make_async_copy(u_all, u_out, save_sem.at[0])
    x_save = pltpu.make_async_copy(x_all, x_out, save_sem.at[1])
    t_save = pltpu.make_async_copy(u_t, t_out, save_sem.at[3])
    u_save.start()
    x_save.start()
    t_save.start()
    wait_all(early(1, 0))
    start_all(early(1, 1))
    wait_all(early(1, 1))

    def loads(k):
        made = []
        for j in COLOURS:
            first, inside, count = unit_range(k, j)
            made.append(pltpu.make_async_copy(
                out.at[:, :, :, pl.ds(first, count)], wbuf.at[k % 2, :, :, :, pl.ds(inside, count)], load_sem.at[k % 2, j]))
        return made

    last = len(CHUNKS) - 1
    give_h = pltpu.make_async_remote_copy(
        src_ref=h_acc.at[pl.ds(tok, tok)], dst_ref=h_other, send_sem=h_sem.at[1], recv_sem=h_sem.at[2],
        device_id=(1 - me_c, me_f), device_id_type=MESH)

    def compute(k):
        n = CHUNKS[k]

        count = x_all.shape[0] // TOK_TILE

        def tile(step, carry):
            t = count - 1 - step
            rows = pl.ds(pl.multiple_of(t * TOK_TILE, TOK_TILE), TOK_TILE)
            w_one, w_three, w_two = chunk_matrices(wbuf[k % 2, :, :, :, 0:CU[k]], n)
            u = u_all[rows, :]
            gate = jnp.dot(u, w_one, preferred_element_type=jnp.float32)
            up = jnp.dot(u, w_three, preferred_element_type=jnp.float32)
            inner = (gate * jax.nn.sigmoid(gate) * up).astype(jnp.bfloat16)
            piece = jnp.dot(inner, w_two, preferred_element_type=jnp.float32)
            h_acc[rows, :] = piece if k == 0 else h_acc[rows, :] + piece
            if k == last:
                pl.when(step == count // 2 - 1)(give_h.start)
            return carry

        repeat(count, tile)

    start_all(late(0, 0))
    start_all(late(1, 0))
    for k in range(last + 1):
        wait_all(late(k, 0))
        start_all(late(k, 1))
        if k + 2 <= last:
            start_all(late(k + 2, 0))
        if k >= 1:
            wait_all(loads(k - 1))
            compute(k - 1)
        wait_all(late(k, 1))
        start_all(loads(k))
    wait_all(loads(last))
    compute(last)
    h_save = pltpu.make_async_copy(h_acc.at[head(tok)], h_mine, h_sem.at[0])
    h_save.start()
    h_save.wait()
    give_h.wait()
    u_save.wait()
    x_save.wait()
    t_save.wait()
    all_sends(True)


def forward_tiles(al13, al2, gain_tile, x_own):
    tok = 2 * x_own.shape[0]
    return pl.pallas_call(
        forward_kernel,
        out_shape=(
            jax.ShapeDtypeStruct((4, 4, 4, UNITS, *UNIT), jnp.bfloat16),
            jax.ShapeDtypeStruct(x_own.shape, jnp.float32),
            jax.ShapeDtypeStruct(x_own.shape, jnp.float32),
            jax.ShapeDtypeStruct((tok, D), jnp.bfloat16),
            jax.ShapeDtypeStruct((D, tok), jnp.bfloat16),
            jax.ShapeDtypeStruct((tok, D), jnp.bfloat16),
        ),
        in_specs=[pl.BlockSpec(memory_space=pltpu.VMEM)] * 3 + [pl.BlockSpec(memory_space=pl.ANY)],
        out_specs=[pl.BlockSpec(memory_space=pl.ANY)] * 6,
        scratch_shapes=[
            pltpu.VMEM((CSLOTS, *TILE), jnp.float32),
            pltpu.VMEM((UNITS, *UNIT), jnp.bfloat16),
            pltpu.VMEM(TILE, jnp.float32),
            pltpu.VMEM((tok, D), jnp.bfloat16),
            pltpu.VMEM((tok, D), jnp.bfloat16),
            pltpu.VMEM((D, tok), jnp.bfloat16),
            pltpu.VMEM((tok, D), jnp.float32),
            pltpu.VMEM((2, 4, 4, 4, max(CU), *UNIT), jnp.bfloat16),
            pltpu.SemaphoreType.DMA((3,)),
            pltpu.SemaphoreType.DMA((15,)),
            pltpu.SemaphoreType.DMA,
            pltpu.SemaphoreType.DMA((len(CHUNKS),)),
            pltpu.SemaphoreType.DMA,
            pltpu.SemaphoreType.DMA((3,)),
            pltpu.SemaphoreType.DMA,
            pltpu.SemaphoreType.DMA((2, 3)),
            pltpu.SemaphoreType.DMA((4,)),
            pltpu.SemaphoreType.DMA((3,)),
            pltpu.SemaphoreType.DMA((6 + 3 * len(CHUNKS), 2, 2)),
            pltpu.SemaphoreType.DMA((6 + 3 * len(CHUNKS), 2, 2)),
        ],
        compiler_params=pltpu.CompilerParams(has_side_effects=True, vmem_limit_bytes=60 * 2 ** 20),
        name='forward_tiles',
    )(al13, al2, gain_tile, x_own)


def cut_tiles(i):
    sizes = [(TPD[ORDER[i]] + 2 - (i + j) % 3) // 3 for j in COLOURS]
    return tuple((sum(sizes[:j]), sizes[j]) for j in COLOURS)


def nt(a, b):
    return lax.dot_general(a, b, (((1,), (1,)), ((), ())), preferred_element_type=jnp.float32)


def backward_kernel(units, u_hbm, t_hbm, x_hbm, e_mine, e_other, loss_tile, out13, out2, out_gain,
                    total, relay0, relay1, relay2, merge0, merge1, merge2, ring_sum, final, wbuf, u_all, u_t, x_all, e_all, r_all,
                    d_gate, d_up, inner, gain_acc,
                    load_sem, w_sem, send_sem, recv_sem, send_tile, send_gain, recv13, recv2, recv_gain, credit):
    dev = my_index()
    me_c = lax.axis_index('dp')
    me_f = lax.axis_index('fsdp')
    pos = ring_pos()
    relays = (relay0, relay1, relay2)
    merges = (merge0, merge1, merge2)
    tok = u_all.shape[0]

    def weight_loads(i):
        k = ORDER[i]
        made = []
        for j in COLOURS:
            first, inside, count = unit_range(k, j)
            made.append(pltpu.make_async_copy(
                units.at[:, :, :, pl.ds(first, count)], wbuf.at[i % 2, :, :, :, pl.ds(inside, count)], w_sem.at[i % 2, j]))
        return made

    def start_all(copies):
        for copy in copies:
            copy.start()

    def wait_all(copies):
        for copy in copies:
            copy.wait()

    inputs = [pltpu.make_async_copy(src, dst, load_sem.at[i])
              for i, (src, dst) in enumerate((
                  (u_hbm, u_all), (e_mine, e_all.at[head(tok // 2)]), (e_other, e_all.at[pl.ds(tok // 2, tok // 2)]),
                  (x_hbm, x_all), (t_hbm, u_t)))]
    start_all(weight_loads(0))
    start_all(inputs)

    def axis_of(colour, phase):
        return AXES[(colour + phase) % 3]

    def set_ref(i, colour, phase, at, rows):
        first = axis_of(colour, 0)
        tiles = (pl.ds(*rows),)
        if phase == 0:
            return total.at[(i % 2,) + tuple(at if a == first else slice(None) for a in AXES) + tiles]
        fixed = {axis_of(colour, q): pos[axis_of(colour, q)] for q in range(phase)}
        fixed[axis_of(colour, phase)] = at
        spot = tuple(fixed.get(a, slice(None)) for a in AXES if a != first)
        return ring_sum.at[(i % 3, colour) + spot + (pl.ds(rows[0] - cut_tiles(i)[colour][0], rows[1]),)]

    def rows_of(i, colour, way):
        first, size = cut_tiles(i)[colour]
        half = (size + 1) // 2
        return ((first, half), (first + half, size - half), (first, size))[way]

    def copies(i, colour, phase, step):
        axis = axis_of(colour, phase)
        made = []
        for way, shift in enumerate(WAYS):
            rows = rows_of(i, colour, way if step == 0 else 2)
            at = (pos[axis] + (2 if step == 0 else shift + 4)) % 4
            dst = (relays if step == 0 else merges)[phase]
            lead = (i % 2, colour, way) + (slice(None),) * (2 - phase)
            sem = (i % 2, colour * 3 + phase, step, way)
            made.append(pltpu.make_async_remote_copy(
                src_ref=set_ref(i, colour, phase, at, rows),
                dst_ref=dst.at[lead + (head(rows[1]),)],
                send_sem=send_sem.at[sem],
                recv_sem=recv_sem.at[sem],
                device_id=neighbour(pos, axis, shift),
                device_id_type=MESH,
            ))
        return made

    def add_set(i, colour, phase, at, rows, landed, done):
        src = set_ref(i, colour, phase, at, rows)

        def body(b, carry):
            spot = ((b // 4, b % 4), (b,), ())[phase]
            value = src[spot + (slice(None),)]
            for part in landed:
                value = value + part[spot + (head(rows[1]),)]
            if not done or phase == 1:
                src[spot + (slice(None),)] = value
            elif phase == 0:
                ring_sum[(i % 3, colour) + spot + (head(rows[1]),)] = value
            else:
                final[i, pl.ds(*rows)] = value
            return carry

        repeat(4 ** (2 - phase), body)

    def tell_neighbours(sem):
        for axis in AXES:
            for shift in WAYS:
                pl.semaphore_signal(sem, inc=1, device_id=neighbour(pos, axis, shift), device_id_type=MESH)

    def reduce_step(i, s):
        if s < 3 and i >= 2:
            pl.semaphore_wait(credit.at[s, i - 2], 6)
        for colour in COLOURS:
            if s > 0:
                phase, step = (s - 1) // 2, (s - 1) % 2
                here = pos[axis_of(colour, phase)]
                wait_all(copies(i, colour, phase, step))
                if step == 0:
                    for way, shift in enumerate((1, 3)):
                        add_set(i, colour, phase, (here + shift) % 4, rows_of(i, colour, way), [relays[phase].at[i % 2, colour, way]], False)
                else:
                    add_set(i, colour, phase, here, rows_of(i, colour, 2),
                            [merges[phase].at[i % 2, colour, way] for way in range(2)], True)
            if s < 6:
                start_all(copies(i, colour, s // 2, s % 2))
        if i + 2 < len(ORDER) and s in (1, 2, 6):
            tell_neighbours(credit.at[min(s, 3) - 1, i])
        if s == 6:
            send_home(i, False)

    def send_home(i, waiting):
        k = ORDER[i]
        n = CHUNKS[k]
        own = TPD[k]

        def per_slot(slot, carry):
            p = me_f * own + slot

            @pl.when(p < 2 * DT * n)
            def _():
                q = p // 2
                row = (q // n) * 2 + p % 2
                owner = (8 * row) // 21
                t = row - row_start(owner)
                dst = out13.at[eight(t), HB * me_c + OFFS[k] + q % n, 0]
                move(final.at[i, slot], dst, send_tile.at[i], recv13.at[t], owner // GRP, owner % GRP, waiting)

            @pl.when(p >= 2 * DT * n)
            def _():
                q = (p - 2 * DT * n) // 2
                row = FT * me_c + 16 * OFFS[k] + (q // ND) * 2 + p % 2
                owner = FIRST_W2 + (8 * row + 38) // 114
                t = row - w2_row_start(owner)
                dst = out2.at[eight(t), q % ND, 0]
                move(final.at[i, slot], dst, send_tile.at[i], recv2.at[t], owner // GRP, owner % GRP, waiting)
            return carry

        repeat(jnp.clip(3 * DT * n - me_f * own, 0, own), per_slot)
        if k == 0:
            @pl.when(me_f == GAIN_F)
            def _():
                def per_device(d, carry):
                    move(final.at[i, 0], out_gain.at[me_c], send_gain, recv_gain.at[me_c], d // GRP, d % GRP, waiting)
                    return carry

                repeat(NDEV, per_device)

    def store_tiles(i, first, value):
        own = CU[ORDER[i]]
        count = value.shape[0]
        for f in range(first // own, (first + count + own - 1) // own):
            low, high = max(first, f * own), min(first + count, (f + 1) * own)
            part = value[low - first:high - first].reshape((high - low) * 2, *TILE)
            z, y, x = coords(f)
            total[i % 2, z, y, x, pl.ds((low - f * own) * 2, (high - low) * 2)] = part

    def to_units(matrix):
        blocks = matrix.shape[1] // 128
        cols = [matrix[:, lanes(j)].reshape(-1, 1, *UNIT) for j in range(blocks)]
        return jnp.concatenate(cols, axis=1).reshape(-1, *UNIT)

    def token_tile(i, t, hooks):
        n = CHUNKS[ORDER[i]]
        width = LANES * n
        rows = pl.ds(pl.multiple_of(t * TOK_TILE, TOK_TILE), TOK_TILE)
        w_one, w_three, w_two = chunk_matrices(wbuf[i % 2, :, :, :, 0:CU[ORDER[i]]], n)
        u = u_all[rows, :]
        gate = jnp.dot(u, w_one, preferred_element_type=jnp.float32)
        up = jnp.dot(u, w_three, preferred_element_type=jnp.float32)
        d_inner = nt(e_all[rows, :], w_two)
        sig = jax.nn.sigmoid(gate)
        silu = gate * sig
        inner[rows, 0:width] = (silu * up).astype(jnp.bfloat16)
        dg = (d_inner * up * sig * (1.0 + gate * (1.0 - sig))).astype(jnp.bfloat16)
        du = (d_inner * silu).astype(jnp.bfloat16)
        d_gate[rows, 0:width] = dg
        d_up[rows, 0:width] = du
        q = nt(dg, w_one) + nt(du, w_three)
        x = x_all[rows, :].astype(jnp.float32)
        if i == 0:
            r_all[rows, :] = lax.rsqrt(jnp.mean(x * x, axis=-1, keepdims=True) + RMS_EPS)
        piece = (q * (x * r_all[rows, :])).reshape(TOK_TILE // 8, 8, D)
        gain_acc[...] += jnp.sum(piece, axis=0)
        for at, hook in hooks:
            pl.when(t == at)(hook)

    gain_acc[...] = jnp.zeros_like(gain_acc)
    wait_all(inputs)
    for i in range(len(ORDER)):
        k = ORDER[i]
        n = CHUNKS[k]
        width = LANES * n
        wait_all(weight_loads(i))
        if i + 1 < len(ORDER):
            start_all(weight_loads(i + 1))
        plan = [tuple(map(int, HOOKS[at:at + 3])) for at in range(0, len(HOOKS), 3)]
        hooks = [(at, functools.partial(reduce_step, i - back, s)) for at, back, s in plan if i >= back]

        def tile(t, carry, i=i, hooks=hooks):
            token_tile(i, t, hooks)
            return carry

        repeat(tok // TOK_TILE, tile)
        store_tiles(i, 0, to_units(jnp.dot(u_t[...], d_gate[:, 0:width], preferred_element_type=jnp.float32)))
        store_tiles(i, DU * n, to_units(jnp.dot(u_t[...], d_up[:, 0:width], preferred_element_type=jnp.float32)))
        d_two = lax.dot_general(inner[:, 0:width], e_all[...], (((0,), (0,)), ((), ())), preferred_element_type=jnp.float32)
        store_tiles(i, 2 * DU * n, to_units(d_two))
        if k == 0:
            d_gain = jnp.sum(gain_acc[...], axis=0, keepdims=True)
            rows = [d_gain[:, lanes(j)] for j in range(ND)]
            total[i % 2, 3, 3, 3, 0] = jnp.concatenate(rows + [loss_tile[7:8, :]], axis=0)
        reduce_step(i, 0)

    last = len(ORDER) - 1
    for back, s in zip(DRAIN[::2], DRAIN[1::2]):
        reduce_step(last - int(back), int(s))
    for i in range(len(ORDER)):
        send_home(i, True)

    @pl.when(dev < FIRST_W2)
    def _():
        def wait_row(t, carry):
            part = out13.at[eight(t)]
            pltpu.make_async_copy(part, part, recv13.at[t]).wait()
            return carry

        repeat(row_start(dev + 1) - row_start(dev), wait_row)

    @pl.when(dev >= FIRST_W2)
    def _():
        def wait_row(t, carry):
            part = out2.at[eight(t)]
            pltpu.make_async_copy(part, part, recv2.at[t]).wait()
            return carry

        repeat(w2_row_start(dev + 1) - w2_row_start(dev), wait_row)

    for c in range(2):
        pltpu.make_async_copy(out_gain.at[c], out_gain.at[c], recv_gain.at[c]).wait()


def backward_tiles(units, u, u_t, x, err, err_other, loss_tile):
    tok = u.shape[0]
    width = 128 * max(CHUNKS)
    relays = [pltpu.VMEM((2, 3, 2) + (4,) * (2 - p) + (HALF, *TILE), jnp.float32) for p in COLOURS]
    merges = [pltpu.VMEM((2, 3, 2) + (4,) * (2 - p) + (FULL, *TILE), jnp.float32) for p in COLOURS]
    bf16_act = pltpu.VMEM((tok, D), jnp.bfloat16)
    chunk_act = pltpu.VMEM((tok, width), jnp.bfloat16)
    dma = pltpu.SemaphoreType.DMA
    return pl.pallas_call(
        backward_kernel,
        out_shape=(
            jax.ShapeDtypeStruct((ROWS13, NB, 1, LANES), jnp.float32),
            jax.ShapeDtypeStruct((ROWS2, ND, 1, LANES), jnp.float32),
            jax.ShapeDtypeStruct((2, *TILE), jnp.float32),
        ),
        in_specs=[pl.BlockSpec(memory_space=pl.ANY)] * 6 + [pl.BlockSpec(memory_space=pltpu.VMEM)],
        out_specs=[pl.BlockSpec(memory_space=pl.ANY)] * 3,
        scratch_shapes=[
            pltpu.VMEM((2, 4, 4, 4, max(TPD), *TILE), jnp.float32),
            *relays,
            *merges,
            pltpu.VMEM((3, 3, 4, 4, FULL, *TILE), jnp.float32),
            pltpu.VMEM((len(ORDER), max(TPD), *TILE), jnp.float32),
            pltpu.VMEM((2, 4, 4, 4, max(CU), *UNIT), jnp.bfloat16),
            bf16_act,
            pltpu.VMEM((D, tok), jnp.bfloat16),
            bf16_act,
            bf16_act,
            pltpu.VMEM((tok, 1), jnp.float32),
            chunk_act,
            chunk_act,
            chunk_act,
            pltpu.VMEM((8, D), jnp.float32),
            dma((5,)),
            dma((2, 3)),
            dma((2, 9, 2, 2)),
            dma((2, 9, 2, 2)),
            dma((len(ORDER),)),
            dma,
            dma((3,)),
            dma((15,)),
            dma((2,)),
            pltpu.SemaphoreType.REGULAR((3, len(ORDER))),
        ],
        compiler_params=pltpu.CompilerParams(has_side_effects=True, vmem_limit_bytes=63 * 2 ** 20),
        name='backward_tiles',
    )(units, u, u_t, x, err, err_other, loss_tile)


def region_offset(dev):
    first13 = D + 8 * FF * row_start(dev)
    first2 = W2_START + 8 * D * w2_row_start(dev)
    return jnp.where(dev <= FIRST_W2, first13, first2) - SHARD * dev


def adam_update(master, adam_m, adam_v, grad_mean):
    m_new = BETA_ONE * adam_m + (1.0 - BETA_ONE) * grad_mean
    v_new = BETA_TWO * adam_v + (1.0 - BETA_TWO) * grad_mean * grad_mean
    m_hat = m_new / (1.0 - BETA_ONE ** ADAM_STEP)
    v_hat = v_new / (1.0 - BETA_TWO ** ADAM_STEP)
    master_new = master - LEARN_RATE * (m_hat / (jnp.sqrt(v_hat) + ADAM_EPS) + DECAY_RATE * master)
    return master_new, m_new, v_new


def aligned_region(own):
    dev = my_index()
    ring = [(i, (i - 1) % NDEV) for i in range(NDEV)]
    spill = lax.ppermute(own[:SPILL], ('dp', 'fsdp'), ring)
    start = region_offset(dev)
    longer = jnp.concatenate([own, spill, jnp.zeros((SPILL + AL_LEN - SHARD - SPILL,), jnp.float32)])
    aligned = lax.dynamic_slice(longer, (start,), (AL_LEN,))
    al13 = aligned.reshape(ROWS13, NB, 1, LANES)
    al2 = aligned[:ROWS2 * D].reshape(ROWS2, ND, 1, LANES)
    gain_tile = own[:1024].reshape(1, 8, 1, LANES)
    return al13, al2, gain_tile


def solution(mesh):
    flat_spec = P(None, ('dp', 'fsdp'))
    act_spec = P(None, ('dp', 'fsdp'), None, None)
    swap = [(0, 1), (1, 0)]

    def train_step(master, adam_m, adam_v, inputs, targets):
        token_total = inputs.shape[1] * inputs.shape[2]

        def local_step(master_sh, m_sh, v_sh, x_loc, y_loc):
            dev = my_index()
            tok = x_loc.shape[1] * x_loc.shape[2]
            own = master_sh.reshape(SHARD)
            x_own = x_loc.reshape(tok, D)
            y_own = y_loc.reshape(tok, D)
            al13, al2, gain_tile = aligned_region(own)
            units, h_mine, h_other, normed, normed_t, x_all = forward_tiles(al13, al2, gain_tile, x_own)
            err = x_own.astype(jnp.float32) + (h_mine + h_other) - y_own.astype(jnp.float32)
            loss_sum = 0.5 * jnp.sum(err * err)
            err_b = err.astype(jnp.bfloat16)
            err_other = lax.ppermute(err_b, 'dp', swap)

            loss_tile = jnp.pad(loss_sum.reshape(1), (D, 127)).reshape(TILE)
            out13, out2, out_gain = backward_tiles(units, normed, normed_t, x_all, err_b, err_other, loss_tile)
            sums = (out_gain[0] + out_gain[1]).reshape(1024)
            loss_value = sums[D] / token_total
            flat13 = out13.reshape(AL_LEN)
            flat2 = jnp.pad(out2.reshape(ROWS2 * D), (0, AL_LEN - ROWS2 * D))
            aligned = jnp.where(dev < FIRST_W2, flat13, flat2)
            start = region_offset(dev)
            longer = jnp.concatenate([jnp.zeros((SPILL,), jnp.float32), aligned, jnp.zeros((SPILL,), jnp.float32)])
            spill = lax.dynamic_slice(longer, (SPILL + SHARD - start,), (SPILL,))
            body = lax.dynamic_slice(longer, (SPILL - start,), (SHARD,))
            ring = [(i, (i + 1) % NDEV) for i in range(NDEV)]
            head = lax.ppermute(spill, ('dp', 'fsdp'), ring)
            head = jnp.where(dev == 0, jnp.pad(sums[:D], (0, SPILL - D)), head)
            grad_sum = jnp.where(jnp.arange(SHARD) < start, jnp.pad(head, (0, SHARD - SPILL)), body)
            grad_mean = grad_sum.reshape(1, SHARD) / token_total
            master_new, m_new, v_new = adam_update(master_sh, m_sh, v_sh, grad_mean)
            return master_new, m_new, v_new, loss_value

        return jax.shard_map(local_step, mesh=mesh, in_specs=(flat_spec, flat_spec, flat_spec, act_spec, act_spec), out_specs=(flat_spec, flat_spec, flat_spec, P()), check_vma=False)(master, adam_m, adam_v, inputs, targets)

    return train_step
```
